16 devices in a mesh: rep: 2 (over y, z), dp: 8 (over x, core).
Axes of the slice: x: 4, y: 2, z: 1, core: 2. Of those that a mesh axis runs over, the one named last changes fastest.
The devices are a block of a 4x4x8 slice.
Arguments:
- g_w_gate: bfloat16 [16, 2, 896, 2560], P(('rep', 'dp')), parts along dimension 0
- g_w_up: bfloat16 [16, 2, 896, 2560], P(('rep', 'dp')), parts along dimension 0
- g_w_down: bfloat16 [16, 2, 2560, 896], P(('rep', 'dp')), parts along dimension 0
- w_gate: bfloat16 [2, 896, 2560], replicated
- w_up: bfloat16 [2, 896, 2560], replicated
- w_down: bfloat16 [2, 2560, 896], replicated
- m_w_gate: float32 [2, 896, 2560], P(None, 'dp')
- m_w_up: float32 [2, 896, 2560], P(None, 'dp')
- m_w_down: float32 [2, 2560, 896], P(None, 'dp')
- v_w_gate: float32 [2, 896, 2560], P(None, 'dp')
- v_w_up: float32 [2, 896, 2560], P(None, 'dp')
- v_w_down: float32 [2, 2560, 896], P(None, 'dp')
Outputs:
- output 1: bfloat16 [4, 896, 2560], P('rep'), parts along dimension 0
- output 2: bfloat16 [4, 896, 2560], P('rep'), parts along dimension 0
- output 3: bfloat16 [4, 2560, 896], P('rep'), parts along dimension 0
- output 4: float32 [4, 896, 2560], P('rep', 'dp'), parts along dimension 0
- output 5: float32 [4, 896, 2560], P('rep', 'dp'), parts along dimension 0
- output 6: float32 [4, 2560, 896], P('rep', 'dp'), parts along dimension 0
- output 7: float32 [4, 896, 2560], P('rep', 'dp'), parts along dimension 0
- output 8: float32 [4, 896, 2560], P('rep', 'dp'), parts along dimension 0
- output 9: float32 [4, 2560, 896], P('rep', 'dp'), parts along dimension 0
There are 2 independent parts. The reference program is written for one: setup_inputs(seed, part) draws one part's arguments, and reference() takes and returns one part's arrays. A program takes and returns all parts, laid end to end along the dimension named above; an argument that names none is the same for every part.
All inputs are finite; a program needn't handle non-finite values.
Results may differ from the reference program's by a relative error of at most 0.022.
Values are sent between devices in bfloat16 or wider.
A program may use at most 768 MiB of HBM per device.

```python
import jax
import jax.numpy as jnp
from jax import lax

DEVICES = 8
D = 896
FF = 2560
LAYERS = 2
NAMES = ("w_gate", "w_up", "w_down")
SHAPES = {"w_gate": (LAYERS, D, FF), "w_up": (LAYERS, D, FF), "w_down": (LAYERS, FF, D)}


def setup_inputs(seed: int = 0, part: int = 0) -> dict:
    kz, *keys = jax.random.split(jax.random.key(seed), 1 + 5 * len(NAMES))
    loud = 2.0 ** jax.random.uniform(kz, (), jnp.float32, -1.0, 1.0)
    drawn = {}
    for name, key, both in zip(NAMES, keys[:3], keys[3:6], strict=True):
        own = jax.random.normal(jax.random.fold_in(key, part), (DEVICES, *SHAPES[name]), jnp.float32)
        shared = jax.random.normal(jax.random.fold_in(both, part), SHAPES[name], jnp.float32)
        drawn["g_" + name] = (loud * (0.7 * shared / DEVICES + 0.7 * own * DEVICES**-0.5)).astype(jnp.bfloat16)
    for name, key in zip(NAMES, keys[6:9], strict=True):
        drawn[name] = (jax.random.normal(key, SHAPES[name], jnp.float32) * SHAPES[name][1] ** -0.5).astype(jnp.bfloat16)
    for name, key in zip(NAMES, keys[9:12], strict=True):
        drawn["m_" + name] = loud * 0.5 * jax.random.normal(key, SHAPES[name], jnp.float32)
    for name, key in zip(NAMES, keys[12:15], strict=True):
        drawn["v_" + name] = loud * loud * jax.random.uniform(key, SHAPES[name], jnp.float32, 0.5, 1.5)
    return drawn


def adamw(w, m, v, g):
    m = 0.9 * m + 0.1 * g
    v = 0.95 * v + 0.05 * g * g
    step = m * lax.rsqrt(v + 1e-8) + 0.1 * w
    return (w - 0.02 * step).astype(jnp.bfloat16), m, v


def clipped(gradients, sum_of_squares, count):
    factor = jnp.minimum(1.0, 0.5 * lax.rsqrt(sum_of_squares / count + 1e-30))
    return [g * factor for g in gradients]


def reference(g_w_gate, g_w_up, g_w_down, w_gate, w_up, w_down, m_w_gate, m_w_up, m_w_down, v_w_gate, v_w_up, v_w_down):
    def total(terms):
        return lax.scan(lambda so_far, term: (so_far + term.astype(jnp.float32), None), jnp.zeros(terms.shape[1:], jnp.float32), terms)[0]

    gradients = [total(terms).astype(jnp.bfloat16).astype(jnp.float32) for terms in (g_w_gate, g_w_up, g_w_down)]
    gradients = clipped(gradients, sum(jnp.sum(g * g) for g in gradients), sum(g.size for g in gradients))
    new = [
        adamw(w.astype(jnp.float32), m, v, g)
        for w, m, v, g in zip((w_gate, w_up, w_down), (m_w_gate, m_w_up, m_w_down), (v_w_gate, v_w_up, v_w_down), gradients, strict=True)
    ]
    return tuple(one[which] for which in range(3) for one in new)
```

```python
import functools

import jax
import jax.numpy as jnp
from jax import lax
from jax.experimental import pallas as pl
from jax.experimental.pallas import tpu as pltpu
from jax.sharding import PartitionSpec as P

MESH = pl.DeviceIdType.MESH
ROWS = 16
F32, BF16 = jnp.float32, jnp.bfloat16
LAYERS = (0, 1)


def chunks_of(units):
    gate, up, down = units
    a, b = gate // 7, 3 * gate // 7
    c, d, e = 12 * down // 20, 17 * down // 20, 19 * down // 20
    return [(0, 0, a), (0, a, b - a), (0, b, gate - b), (1, 0, up), (2, 0, c), (2, c, d - c), (2, d, e - d), (2, e, down - e)]


def kernel(n, count, chunks, *refs):
    g, w, m_in, v_in = refs[0:3], refs[3:6], refs[6:9], refs[9:12]
    new, m, v = refs[12:15], refs[15:18], refs[18:21]
    own, old = refs[21:24], refs[24:27]
    total, squares = refs[27:29]
    (d2d_send, d2d_recv, ici_send, ici_recv, load_sem, state_sem, sq_send, sq_recv) = refs[29:]

    me = lax.axis_index("dp")
    chip, core = me // 2, me % 2
    chips = n // 2
    partner = chip * 2 + 1 - core
    down_, up_, far = (chip + chips - 1) % chips, (chip + 1) % chips, (chip + 2) % chips
    sides = (down_, up_)

    def at(c):
        return c * 2 + core

    def remote(src, dst, send, recv, to):
        return pltpu.make_async_remote_copy(src_ref=src, dst_ref=dst, send_sem=send, recv_sem=recv, device_id={"dp": to}, device_id_type=MESH)

    blocks = ((far, far), (up_, down_), (down_, up_), (chip, chip))
    target = ((down_, up_), (up_, down_), (down_, up_))

    def load(p, l, t):
        return pltpu.make_async_copy(g[t].at[l, at(blocks[p][l])], own[t].at[l], load_sem.at[l, t])

    def state():
        return [
            copy
            for t in range(3)
            for copy in (
                pltpu.make_async_copy(w[t].at[:, me], old[t], state_sem.at[0, t]),
                pltpu.make_async_copy(m_in[t], m[t], state_sem.at[1, t]),
                pltpu.make_async_copy(v_in[t], v[t], state_sem.at[2, t]),
            )
        ]

    for t in range(3):
        for l in LAYERS:
            load(0, l, t).start()

    barrier = pltpu.get_barrier_semaphore()
    for k in range(1, n):
        pl.semaphore_signal(barrier, inc=1, device_id={"dp": (me + k) % n}, device_id_type=MESH)
    pl.semaphore_wait(barrier, n - 1)

    def handed(p, l, i):
        t, s, size = chunks[i]
        there = blocks[p][l] * 2 + 1 - core
        part = (l, there, pl.ds(s, size))
        return remote(g[t].at[part], new[t].at[part], d2d_send.at[p, l, i], d2d_recv.at[p, l, i], partner)

    for p in range(4):
        for i in range(len(chunks)):
            for l in LAYERS:
                handed(p, l, i).start()

    def inbox(j):
        return j * 2 + 1 - core

    def passed(p, l, i):
        t, s, size = chunks[i]
        return remote(
            new[t].at[l, at(blocks[p][l]), pl.ds(s, size)],
            new[t].at[l, inbox(p), pl.ds(s, size)],
            ici_send.at[p, l, i],
            ici_recv.at[p, l, i],
            at(target[p][l]),
        )

    total[...] = jnp.zeros_like(total)

    def add(p, l, i):
        t, s, size = chunks[i]
        block = at(blocks[p][l])

        @pl.loop(s, s + size)
        def _(r):
            x = own[t][l, r].astype(F32) + new[t][l, block, r].astype(F32)
            if p == 2:
                x = x + new[t][l, inbox(0), r].astype(F32)
            if p == 3:
                x = x + new[t][l, inbox(1), r].astype(F32) + new[t][l, inbox(2), r].astype(F32)
            x = x.astype(BF16)
            new[t][l, block, r] = x
            if p == 3:
                x = x.astype(F32)
                x = x * x
                parts = [x[:, k : k + 128] for k in range(0, x.shape[1], 128)]
                while len(parts) > 1:
                    parts = [a + b for a, b in zip(parts[::2], parts[1::2])] + ([parts[-1]] if len(parts) % 2 else [])
                total[...] += parts[0]

    for p in range(4):
        for i, (t, s, size) in enumerate(chunks):
            for l in LAYERS:
                if s == 0:
                    load(p, l, t).wait()
                handed(p, l, i).wait_recv()
                if p == 2:
                    passed(0, l, i).wait_recv()
                if p == 3:
                    passed(1, l, i).wait_recv()
                    passed(2, l, i).wait_recv()
                add(p, l, i)
                if p < 3:
                    passed(p, l, i).start()
                    if s + size == g[t].shape[2]:
                        load(p + 1, l, t).start()
        if p == 2:
            for copy in state():
                copy.start()

    for p in range(4):
        for i in range(len(chunks)):
            for l in LAYERS:
                handed(p, l, i).wait_send()
                if p < 3:
                    passed(p, l, i).wait_send()

    def told(k):
        return remote(squares.at[me], squares.at[me], sq_send.at[k], sq_recv.at[k], (me + k) % n)

    squares[me] = total[...]
    for k in range(1, n):
        told(k).start()
    for copy in state():
        copy.wait()
    for k in range(1, n):
        told(k).wait_recv()
    everything = squares[0]
    for k in range(1, n):
        everything = everything + squares[k]
    everything = jnp.sum(everything, axis=(0, 1), keepdims=True)
    factor = jnp.minimum(1.0, 0.5 * lax.rsqrt(everything / count + 1e-30))

    def spread(q, l, i):
        t, s, size = chunks[i]
        block = (chip, chip, sides[l])[q]
        part = (l, at(block), pl.ds(s, size))
        to = (sides[1 - l], sides[l], sides[1 - l])[q]
        return remote(new[t].at[part], new[t].at[part], ici_send.at[q, l, i], ici_recv.at[q, l, i], at(to))

    def came(q, l):
        return (sides[l], sides[1 - l], far)[q]

    def share(q, l, i):
        t, s, size = chunks[i]
        block = chip if q == 0 else came(q - 1, l)
        part = (l, at(block), pl.ds(s, size))
        return remote(new[t].at[part], new[t].at[part], d2d_send.at[q, l, i], d2d_recv.at[q, l, i], partner)

    for i, (t, s, size) in enumerate(chunks):
        for l in LAYERS:

            @pl.loop(s, s + size)
            def _(r, t=t, l=l):
                grad = new[t][l, me, r].astype(F32) * factor
                m1 = 0.9 * m[t][l, r] + 0.1 * grad
                v1 = 0.95 * v[t][l, r] + 0.05 * grad * grad
                w0 = old[t][l, r].astype(F32)
                step = m1 * lax.rsqrt(v1 + 1e-8) + 0.1 * w0
                new[t][l, me, r] = (w0 - 0.02 * step).astype(BF16)
                m[t][l, r] = m1
                v[t][l, r] = v1

            spread(0, l, i).start()
            share(0, l, i).start()
    for i in range(len(chunks)):
        for l in LAYERS:
            spread(1, l, i).start()
    for q in range(3):
        for i in range(len(chunks)):
            for l in LAYERS:
                spread(q, l, i).wait_recv()
                if q == 0:
                    spread(2, l, i).start()
                share(q + 1, l, i).start()
    for q in range(4):
        for i in range(len(chunks)):
            for l in LAYERS:
                share(q, l, i).wait_recv()
    for q in range(4):
        for i in range(len(chunks)):
            for l in LAYERS:
                share(q, l, i).wait_send()
                if q < 3:
                    spread(q, l, i).wait_send()
    for k in range(1, n):
        told(k).wait_send()


def put_out(*refs):
    copies = [pltpu.make_async_copy(refs[i], refs[9 + i], refs[18].at[i]) for i in range(9)]
    for copy in copies:
        copy.start()
    for copy in copies:
        copy.wait()


OUT = pltpu.VMEM


def solution(mesh):
    n = mesh.shape["dp"]

    def step(*arrays):
        terms, weights, ms, vs = (arrays[i : i + 3] for i in (0, 3, 6, 9))
        layers = weights[0].shape[0]
        units = [one.shape[1] // ROWS for one in ms]
        cols = [one.shape[2] for one in ms]
        chunks = chunks_of(units)
        count = n * sum(one.size for one in ms)
        whole = [(layers, n, u, ROWS, c) for u, c in zip(units, cols)]
        part = [(layers, u, ROWS, c) for u, c in zip(units, cols)]
        operands = (
            [t.reshape(s) for t, s in zip(terms, whole)]
            + [x.reshape(s) for x, s in zip(weights, whole)]
            + [x.reshape(s) for x, s in zip(ms, part)]
            + [x.reshape(s) for x, s in zip(vs, part)]
        )
        k = len(chunks)
        dma = pltpu.SemaphoreType.DMA
        outs = pl.pallas_call(
            functools.partial(kernel, n, count, chunks),
            name="step",
            out_shape=[OUT(s, BF16) for s in whole] + [OUT(s, F32) for s in part] * 2,
            in_specs=[pl.BlockSpec(memory_space=pltpu.HBM)] * 12,
            out_specs=[pl.BlockSpec(memory_space=OUT)] * 9,
            scratch_shapes=[pltpu.VMEM((2, *s[1:]), BF16) for s in part]
            + [pltpu.VMEM(s, BF16) for s in part]
            + [pltpu.VMEM((ROWS, 128), F32), pltpu.VMEM((n, ROWS, 128), F32)]
            + [dma((4, 2, k)), dma((4, 2, k)), dma((3, 2, k)), dma((3, 2, k)), dma((2, 3)), dma((3, 3)), dma((n,)), dma((n,))],
            compiler_params=pltpu.CompilerParams(collective_id=0, has_side_effects=True, vmem_limit_bytes=LIMIT),
        )(*[pltpu.with_memory_space_constraint(o, pltpu.HBM) for o in operands])
        outs = pl.pallas_call(
            put_out,
            name="put_out",
            out_shape=[pltpu.HBM(s, BF16) for s in whole] + [pltpu.HBM(s, F32) for s in part] * 2,
            in_specs=[pl.BlockSpec(memory_space=OUT)] * 9,
            out_specs=[pl.BlockSpec(memory_space=pltpu.HBM)] * 9,
            scratch_shapes=[dma((9,))],
            compiler_params=pltpu.CompilerParams(has_side_effects=True, vmem_limit_bytes=2**20),
        )(*outs)
        shapes = [x.shape for x in weights] + [x.shape for x in ms] * 2
        return tuple(o.reshape(s) for o, s in zip(outs, shapes))

    all_of, cut = P(None, None, None), P(None, "dp", None)
    return jax.shard_map(
        step,
        mesh=mesh,
        in_specs=(P(("rep", "dp"), None, None, None),) * 3 + (all_of,) * 3 + (cut,) * 6,
        out_specs=(P("rep", None, None),) * 3 + (P("rep", "dp", None),) * 6,
        check_vma=False,
    )


LIMIT = 8 * 2**20
```

```python
import functools

import jax
import jax.numpy as jnp
from jax import lax
from jax.experimental import pallas as pl
from jax.experimental.pallas import tpu as pltpu
from jax.sharding import PartitionSpec as P

MESH = pl.DeviceIdType.MESH
ROWS = 16
VMEM_LIMIT = 8 * 2**20
F32, BF16 = jnp.float32, jnp.bfloat16
LAYERS = (0, 1)


def chunks_of(units):
    gate, up, down = units
    a, b = gate // 7, 3 * gate // 7
    head = [(0, 0, a), (0, a, b - a), (0, b, gate - b)]
    c, d, e = 12 * down // 20, 17 * down // 20, 19 * down // 20
    sums = head + [(1, 0, up), (2, 0, c), (2, c, d - c), (2, d, e - d), (2, e, down - e)]
    c, d, e = down // 10, 3 * down // 20, down // 5
    news = head + [(2, e, down - e), (1, 0, up), (2, 0, c), (2, c, d - c), (2, d, e - d)]
    return sums, news


def kernel(n, count, sums, news, *refs):
    g, w, m_in, v_in = refs[0:3], refs[3:6], refs[6:9], refs[9:12]
    new, m, v = refs[12:15], refs[15:18], refs[18:21]
    piece = refs[21:23]
    own, old = refs[23:26], refs[26:29]
    total, squares = refs[29:31]
    (d2d_send, d2d_recv, ici_send, ici_recv, load_sem, state_sem, sq_send, sq_recv, piece_sem) = refs[31:]

    me = lax.axis_index("dp")
    chip, core = me // 2, me % 2
    chips = n // 2
    partner = chip * 2 + 1 - core
    down_, up_, far = (chip + chips - 1) % chips, (chip + 1) % chips, (chip + 2) % chips
    sides = (down_, up_)

    def at(c):
        return c * 2 + core

    def remote(src, dst, send, recv, to):
        return pltpu.make_async_remote_copy(src_ref=src, dst_ref=dst, send_sem=send, recv_sem=recv, device_id={"dp": to}, device_id_type=MESH)

    blocks = ((far, far), (up_, down_), (down_, up_), (chip, chip))
    target = ((down_, up_), (up_, down_), (down_, up_))

    def load(p, l, t):
        return pltpu.make_async_copy(g[t].at[l, at(blocks[p][l])], own[t].at[l], load_sem.at[l, t])

    def state():
        return [
            copy
            for t in range(3)
            for copy in (
                pltpu.make_async_copy(w[t].at[:, me], old[t], state_sem.at[0, t]),
                pltpu.make_async_copy(m_in[t], m[t], state_sem.at[1, t]),
                pltpu.make_async_copy(v_in[t], v[t], state_sem.at[2, t]),
            )
        ]

    for t in range(3):
        for l in LAYERS:
            load(0, l, t).start()

    barrier = pltpu.get_barrier_semaphore()
    for k in range(1, n):
        pl.semaphore_signal(barrier, inc=1, device_id={"dp": (me + k) % n}, device_id_type=MESH)
    pl.semaphore_wait(barrier, n - 1)

    def handed(p, l, i):
        t, s, size = sums[i]
        there = blocks[p][l] * 2 + 1 - core
        part = (l, there, pl.ds(s, size))
        return remote(g[t].at[part], new[t].at[part], d2d_send.at[0, t], d2d_recv.at[p, l, i], partner)

    for p in range(4):
        for i in range(len(sums)):
            for l in LAYERS:
                handed(p, l, i).start()

    def inbox(j):
        return j * 2 + 1 - core

    def passed(p, l, i):
        t, s, size = sums[i]
        return remote(
            new[t].at[l, at(blocks[p][l]), pl.ds(s, size)],
            new[t].at[l, inbox(p), pl.ds(s, size)],
            ici_send.at[0, t],
            ici_recv.at[p, l, i],
            at(target[p][l]),
        )

    total[...] = jnp.zeros_like(total)

    def add(p, l, i):
        t, s, size = sums[i]
        block = at(blocks[p][l])

        @pl.loop(s, s + size)
        def _(r):
            x = own[t][l, r].astype(F32) + new[t][l, block, r].astype(F32)
            if p == 2:
                x = x + new[t][l, inbox(0), r].astype(F32)
            if p == 3:
                x = x + new[t][l, inbox(1), r].astype(F32) + new[t][l, inbox(2), r].astype(F32)
            x = x.astype(BF16)
            new[t][l, block, r] = x
            if p == 3:
                x = x.astype(F32)
                x = x * x
                parts = [x[:, k : k + 128] for k in range(0, x.shape[1], 128)]
                while len(parts) > 1:
                    parts = [a + b for a, b in zip(parts[::2], parts[1::2])] + ([parts[-1]] if len(parts) % 2 else [])
                total[...] += parts[0]

    for p in range(4):
        for i, (t, s, size) in enumerate(sums):
            for l in LAYERS:
                if s == 0:
                    load(p, l, t).wait()
                handed(p, l, i).wait_recv()
                if p == 2:
                    passed(0, l, i).wait_recv()
                if p == 3:
                    passed(1, l, i).wait_recv()
                    passed(2, l, i).wait_recv()
                add(p, l, i)
                if p < 3:
                    passed(p, l, i).start()
                    if s + size == g[t].shape[2]:
                        load(p + 1, l, t).start()
        if p == 2:
            for copy in state():
                copy.start()

    def sent(t, blocks, sem):
        part = new[t].at[:, pl.ds(0, blocks)]
        pltpu.make_async_copy(part, part, sem).wait()

    for t in range(3):
        sent(t, 4, d2d_send.at[0, t])
        sent(t, 3, ici_send.at[0, t])

    def told(k):
        return remote(squares.at[me], squares.at[me], sq_send.at[k], sq_recv.at[k], (me + k) % n)

    squares[me] = jnp.sum(total[...], axis=0, keepdims=True)
    for k in range(1, n):
        told(k).start()
    for copy in state():
        copy.wait()
    for k in range(1, n):
        told(k).wait_recv()
    everything = squares[0]
    for k in range(1, n):
        everything = everything + squares[k]
    everything = jnp.sum(everything, axis=(0, 1), keepdims=True)
    factor = jnp.minimum(1.0, 0.5 * lax.rsqrt(everything / count + 1e-30))

    rest = news[3]

    def spread(q, l, i):
        t, s, size = news[i]
        block = (chip, chip, sides[l])[q]
        part = (l, at(block), pl.ds(s, size))
        to = (sides[1 - l], sides[l], sides[1 - l])[q]
        return remote(new[t].at[part], new[t].at[part], ici_send.at[q // 2, t], ici_recv.at[q, l, i], at(to))

    def came(q, l):
        return (sides[l], sides[1 - l], far)[q]

    def share(q, l, i):
        t, s, size = news[i]
        block = chip if q == 0 else came(q - 1, l)
        part = (l, at(block), pl.ds(s, size))
        arrived = d2d_recv.at[3, l, i] if q == 3 else d2d_recv.at[0, 0, t]
        return remote(new[t].at[part], new[t].at[part], d2d_send.at[q // 3, t], arrived, partner)

    def keep(l):
        t, s, size = rest
        return pltpu.make_async_copy(new[t].at[l, at(sides[l]), pl.ds(s, size)], piece[l], piece_sem.at[l])

    for i, (t, s, size) in enumerate(news):
        for l in LAYERS:

            @pl.loop(s, s + size)
            def _(r, t=t, l=l):
                grad = new[t][l, me, r].astype(F32) * factor
                m1 = 0.9 * m[t][l, r] + 0.1 * grad
                v1 = 0.95 * v[t][l, r] + 0.05 * grad * grad
                w0 = old[t][l, r].astype(F32)
                step = m1 * lax.rsqrt(v1 + 1e-8) + 0.1 * w0
                new[t][l, me, r] = (w0 - 0.02 * step).astype(BF16)
                m[t][l, r] = m1
                v[t][l, r] = v1

            spread(0, l, i).start()
            share(0, l, i).start()
    for i in range(len(news)):
        for l in LAYERS:
            spread(1, l, i).start()
    for k in range(1, n):
        told(k).wait_send()
    for q in range(3):
        for i in range(len(news)):
            for l in LAYERS:
                if q == 2 and news[i] == rest:
                    continue
                spread(q, l, i).wait_recv()
                if q == 0 and news[i] == rest:
                    keep(l).start()
                elif q == 0:
                    spread(2, l, i).start()
                share(q + 1, l, i).start()
        if q == 1:
            for l in LAYERS:
                keep(l).wait()
            for t in range(3):
                sent(t, 2, ici_send.at[0, t])
    for t in range(3):
        sent(t, 3, d2d_recv.at[0, 0, t])
        sent(t, 3, d2d_send.at[0, t])
    for i in range(len(news)):
        for l in LAYERS:
            if news[i] != rest:
                share(3, l, i).wait_recv()
    for t in range(3):
        units = rest[1] if t == rest[0] else new[t].shape[2]
        part = new[t].at[:, pl.ds(0, 1), pl.ds(0, units)]
        pltpu.make_async_copy(part, part, d2d_send.at[1, t]).wait()
        pltpu.make_async_copy(part, part, ici_send.at[1, t]).wait()


def put_out(k, *refs):
    copies = [pltpu.make_async_copy(refs[i], refs[k + i], refs[2 * k].at[i]) for i in range(k)]
    for copy in copies:
        copy.start()
    for copy in copies:
        copy.wait()


def written(name, *arrays):
    k = len(arrays)
    size = sum(a.size * a.dtype.itemsize for a in arrays)
    return pl.pallas_call(
        functools.partial(put_out, k),
        name=name,
        out_shape=[pltpu.HBM(a.shape, a.dtype) for a in arrays],
        in_specs=[IN_VMEM] * k,
        out_specs=[IN_HBM] * k,
        scratch_shapes=[pltpu.SemaphoreType.DMA((k,))],
        cost_estimate=pl.CostEstimate(flops=100 * size, bytes_accessed=size, transcendentals=0),
        compiler_params=pltpu.CompilerParams(has_side_effects=True, vmem_limit_bytes=VMEM_LIMIT),
    )(*arrays)


def patch(n, down, *refs):
    parts, out, sem = refs[:4], refs[4], refs[5]
    me = lax.axis_index("dp")
    far, core = (me // 2 + 2) % (n // 2), me % 2
    first = out.shape[2] - parts[0].shape[0]
    copies = []
    for i, part in enumerate(parts):
        block = far * 2 + (core if i < 2 else 1 - core)
        copies.append(pltpu.make_async_copy(part, out.at[i % 2, block, pl.ds(first, part.shape[0])], sem.at[i]))
    for copy in copies:
        copy.start()
    for copy in copies:
        copy.wait()


IN_VMEM, IN_HBM = pl.BlockSpec(memory_space=pltpu.VMEM), pl.BlockSpec(memory_space=pltpu.HBM)


def solution(mesh):
    n = mesh.shape["dp"]
    chips = n // 2
    ring = [(2 * c + k, 2 * ((c + 1) % chips) + k) for c in range(chips) for k in range(2)]
    back = [(b, a) for a, b in ring]
    swap = [(d, d + 1 - 2 * (d % 2)) for d in range(n)]

    def step(*arrays):
        terms, weights, ms, vs = (arrays[i : i + 3] for i in (0, 3, 6, 9))
        layers = weights[0].shape[0]
        units = [one.shape[1] // ROWS for one in ms]
        cols = [one.shape[2] for one in ms]
        sums, news = chunks_of(units)
        count = n * sum(one.size for one in ms)
        whole = [(layers, n, u, ROWS, c) for u, c in zip(units, cols)]
        part = [(layers, u, ROWS, c) for u, c in zip(units, cols)]
        left = (news[3][2], ROWS, cols[2])
        operands = (
            [t.reshape(s) for t, s in zip(terms, whole)]
            + [x.reshape(s) for x, s in zip(weights, whole)]
            + [x.reshape(s) for x, s in zip(ms, part)]
            + [x.reshape(s) for x, s in zip(vs, part)]
        )
        k = max(len(sums), len(news))
        dma = pltpu.SemaphoreType.DMA
        outs = pl.pallas_call(
            functools.partial(kernel, n, count, sums, news),
            name="step",
            out_shape=[pltpu.VMEM(s, BF16) for s in whole] + [pltpu.VMEM(s, F32) for s in part] * 2 + [pltpu.HBM(left, BF16)] * 2,
            in_specs=[IN_HBM] * 12,
            out_specs=[IN_VMEM] * 9 + [IN_HBM] * 2,
            scratch_shapes=[pltpu.VMEM((2, *s[1:]), BF16) for s in part]
            + [pltpu.VMEM(s, BF16) for s in part]
            + [pltpu.VMEM((ROWS, 128), F32), pltpu.VMEM((n, 1, 128), F32)]
            + [dma((2, 3)), dma((4, 2, k)), dma((2, 3)), dma((3, 2, k)), dma((2, 3)), dma((3, 3)), dma((n,)), dma((n,)), dma((2,))],
            compiler_params=pltpu.CompilerParams(collective_id=0, has_side_effects=True, vmem_limit_bytes=VMEM_LIMIT),
        )(*[pltpu.with_memory_space_constraint(o, pltpu.HBM) for o in operands])
        gate, up, down, *moments = outs[:9]
        over = [lax.ppermute(outs[9], "dp", ring), lax.ppermute(outs[10], "dp", back)]
        first = written("put_first", *moments, gate, up)
        over[0], over[1] = lax.optimization_barrier((*over, first[0]))[:2]
        across = [lax.ppermute(o, "dp", swap) for o in over]
        (last,) = written("put_last", down)
        new_down = pl.pallas_call(
            functools.partial(patch, n),
            name="patch",
            out_shape=pltpu.HBM(last.shape, BF16),
            in_specs=[IN_HBM] + [IN_VMEM] * 4,
            out_specs=IN_HBM,
            scratch_shapes=[dma((4,))],
            input_output_aliases={0: 0},
            compiler_params=pltpu.CompilerParams(has_side_effects=True, vmem_limit_bytes=VMEM_LIMIT),
        )(last, *[pltpu.with_memory_space_constraint(o, pltpu.VMEM) for o in over + across])
        outs = (first[6], first[7], new_down, *first[:6])
        shapes = [x.shape for x in weights] + [x.shape for x in ms] * 2
        return tuple(o.reshape(s) for o, s in zip(outs, shapes))

    all_of, cut = P(None, None, None), P(None, "dp", None)
    return jax.shard_map(
        step,
        mesh=mesh,
        in_specs=(P(("rep", "dp"), None, None, None),) * 3 + (all_of,) * 3 + (cut,) * 6,
        out_specs=(P("rep", None, None),) * 3 + (P("rep", "dp", None),) * 6,
        check_vma=False,
    )
```

```python
import functools

import jax
import jax.numpy as jnp
from jax import lax
from jax.experimental import pallas as pl
from jax.experimental.pallas import tpu as pltpu
from jax.sharding import PartitionSpec as P

MESH = pl.DeviceIdType.MESH
ROWS = 16
VMEM_LIMIT = 8 * 2**20
F32, BF16 = jnp.float32, jnp.bfloat16
LAYERS = (0, 1)


def chunks_of(units):
    gate, up, down = units
    a, b = gate // 7, 3 * gate // 7
    c, d, e = 12 * down // 20, 17 * down // 20, 19 * down // 20
    chunks = [(0, 0, a), (0, a, b - a), (0, b, gate - b), (1, 0, up), (2, 0, c), (2, c, d - c), (2, d, e - d), (2, e, down - e)]
    return chunks, (1, 2, 3)


def kernel(n, count, chunks, left, *refs):
    g, w, m_in, v_in = refs[0:3], refs[3:6], refs[6:9], refs[9:12]
    new, m, v = refs[12:15], refs[15:18], refs[18:21]
    piece = refs[21]
    own, old = refs[22:25], refs[25:28]
    total, squares = refs[28:30]
    (d2d_send, d2d_recv, ici_send, ici_recv, load_sem, state_sem, sq_send, sq_recv) = refs[30:]

    me = lax.axis_index("dp")
    chip, core = me // 2, me % 2
    chips = n // 2
    partner = chip * 2 + 1 - core
    down_, up_, far = (chip + chips - 1) % chips, (chip + 1) % chips, (chip + 2) % chips
    sides = (down_, up_)

    def at(c):
        return c * 2 + core

    def remote(src, dst, send, recv, to):
        return pltpu.make_async_remote_copy(src_ref=src, dst_ref=dst, send_sem=send, recv_sem=recv, device_id={"dp": to}, device_id_type=MESH)

    blocks = ((far, far), (up_, down_), (down_, up_), (chip, chip))
    target = ((down_, up_), (up_, down_), (down_, up_))

    def load(p, l, t):
        return pltpu.make_async_copy(g[t].at[l, at(blocks[p][l])], own[t].at[l], load_sem.at[l, t])

    def state():
        return [
            copy
            for t in range(3)
            for copy in (
                pltpu.make_async_copy(w[t].at[:, me], old[t], state_sem.at[0, t]),
                pltpu.make_async_copy(m_in[t], m[t], state_sem.at[1, t]),
                pltpu.make_async_copy(v_in[t], v[t], state_sem.at[2, t]),
            )
        ]

    for t in range(3):
        for l in LAYERS:
            load(0, l, t).start()

    barrier = pltpu.get_barrier_semaphore()
    for k in range(1, n):
        pl.semaphore_signal(barrier, inc=1, device_id={"dp": (me + k) % n}, device_id_type=MESH)
    pl.semaphore_wait(barrier, n - 1)

    def handed(p, l, i):
        t, s, size = chunks[i]
        there = blocks[p][l] * 2 + 1 - core
        part = (l, there, pl.ds(s, size))
        return remote(g[t].at[part], new[t].at[part], d2d_send.at[0, t], d2d_recv.at[p, l, i], partner)

    for p in range(4):
        for i in range(len(chunks)):
            for l in LAYERS:
                handed(p, l, i).start()

    def inbox(j):
        return j * 2 + 1 - core

    def passed(p, l, i):
        t, s, size = chunks[i]
        return remote(
            new[t].at[l, at(blocks[p][l]), pl.ds(s, size)],
            new[t].at[l, inbox(p), pl.ds(s, size)],
            ici_send.at[0, t],
            ici_recv.at[p, l, i],
            at(target[p][l]),
        )

    total[...] = jnp.zeros_like(total)

    def add(p, l, i):
        t, s, size = chunks[i]
        block = at(blocks[p][l])

        @pl.loop(s, s + size)
        def _(r):
            x = own[t][l, r].astype(F32) + new[t][l, block, r].astype(F32)
            if p == 2:
                x = x + new[t][l, inbox(0), r].astype(F32)
            if p == 3:
                x = x + new[t][l, inbox(1), r].astype(F32) + new[t][l, inbox(2), r].astype(F32)
            x = x.astype(BF16)
            new[t][l, block, r] = x
            if p == 3:
                x = x.astype(F32)
                x = x * x
                parts = [x[:, k : k + 128] for k in range(0, x.shape[1], 128)]
                while len(parts) > 1:
                    parts = [a + b for a, b in zip(parts[::2], parts[1::2])] + ([parts[-1]] if len(parts) % 2 else [])
                total[...] += parts[0]

    for p in range(4):
        for i, (t, s, size) in enumerate(chunks):
            for l in LAYERS:
                if s == 0:
                    load(p, l, t).wait()
                handed(p, l, i).wait_recv()
                if p == 2:
                    passed(0, l, i).wait_recv()
                if p == 3:
                    passed(1, l, i).wait_recv()
                    passed(2, l, i).wait_recv()
                add(p, l, i)
                if p < 3:
                    passed(p, l, i).start()
                    if s + size == g[t].shape[2]:
                        load(p + 1, l, t).start()
        if p == 2:
            for copy in state():
                copy.start()

    def sent(t, blocks, sem):
        part = new[t].at[:, pl.ds(0, blocks)]
        pltpu.make_async_copy(part, part, sem).wait()

    for t in range(3):
        sent(t, 4, d2d_send.at[0, t])
        sent(t, 3, ici_send.at[0, t])

    def told(k):
        return remote(squares.at[me], squares.at[me], sq_send.at[k], sq_recv.at[k], (me + k) % n)

    squares[me] = jnp.sum(total[...], axis=0, keepdims=True)
    for k in range(1, n):
        told(k).start()
    for copy in state():
        copy.wait()
    for k in range(1, n):
        told(k).wait_recv()
    everything = squares[0]
    for k in range(1, n):
        everything = everything + squares[k]
    everything = jnp.sum(everything, axis=(0, 1), keepdims=True)
    factor = jnp.minimum(1.0, 0.5 * lax.rsqrt(everything / count + 1e-30))

    def kind(q, last, i):
        return 0 if q < last else 2 if i in left else 1

    def spread(q, l, i):
        t, s, size = chunks[i]
        block = (chip, chip, sides[l])[q]
        part = (l, at(block), pl.ds(s, size))
        to = (sides[1 - l], sides[l], sides[1 - l])[q]
        return remote(new[t].at[part], new[t].at[part], ici_send.at[kind(q, 2, i), t], ici_recv.at[q, l, i], at(to))

    def came(q, l):
        return (sides[l], sides[1 - l], far)[q]

    def share(q, l, i):
        t, s, size = chunks[i]
        block = chip if q == 0 else came(q - 1, l)
        part = (l, at(block), pl.ds(s, size))
        arrived = d2d_recv.at[3, l, i] if q == 3 else d2d_recv.at[0, 0, t]
        return remote(new[t].at[part], new[t].at[part], d2d_send.at[kind(q, 3, i), t], arrived, partner)

    def keep(l, i):
        t, s, size = chunks[i]
        first = sum(chunks[k][2] for k in left if k < i)

        @pl.loop(0, size)
        def _(r):
            piece[first + r] = new[t][l, at(sides[l]), s + r]

    def passes(l, i, action):
        if i in left:
            pl.when(core != l)(action)
        else:
            action()

    for i, (t, s, size) in enumerate(chunks):
        for l in LAYERS:

            @pl.loop(s, s + size)
            def _(r, t=t, l=l):
                grad = new[t][l, me, r].astype(F32) * factor
                m1 = 0.9 * m[t][l, r] + 0.1 * grad
                v1 = 0.95 * v[t][l, r] + 0.05 * grad * grad
                w0 = old[t][l, r].astype(F32)
                step = m1 * lax.rsqrt(v1 + 1e-8) + 0.1 * w0
                new[t][l, me, r] = (w0 - 0.02 * step).astype(BF16)
                m[t][l, r] = m1
                v[t][l, r] = v1

            spread(0, l, i).start()
            share(0, l, i).start()
    for i in range(len(chunks)):
        for l in LAYERS:
            spread(1, l, i).start()
    for k in range(1, n):
        told(k).wait_send()
    for q in range(3):
        for i in range(len(chunks)):
            for l in LAYERS:

                def arrival(q=q, l=l, i=i):
                    spread(q, l, i).wait_recv()
                    share(q + 1, l, i).start()

                if q < 2:
                    spread(q, l, i).wait_recv()
                    if q == 0:
                        passes(l, i, lambda l=l, i=i: spread(2, l, i).start())
                    share(q + 1, l, i).start()
                    if q == 0 and i in left:
                        pl.when(core == l)(lambda l=l, i=i: keep(l, i))
                else:
                    passes(l, i, arrival)
        if q == 1:
            for t in range(3):
                sent(t, 2, ici_send.at[0, t])
    for t in range(3):
        sent(t, 3, d2d_recv.at[0, 0, t])
        sent(t, 3, d2d_send.at[0, t])
    for i in range(len(chunks)):
        for l in LAYERS:
            if i in left:
                pl.when(core == l)(lambda l=l, i=i: share(3, l, i).wait_recv())
            else:
                share(3, l, i).wait_recv()
    for t in range(3):
        units = sum(chunks[i][2] for i in left if chunks[i][0] == t)
        for part, sems in ((new[t].at[:, 0, pl.ds(0, new[t].shape[2] - units)], 1), (new[t].at[0, 0, pl.ds(0, units)], 2)):
            if part.shape[-3]:
                pltpu.make_async_copy(part, part, d2d_send.at[sems, t]).wait()
                pltpu.make_async_copy(part, part, ici_send.at[sems, t]).wait()


def put_out(k, *refs):
    copies = [pltpu.make_async_copy(refs[i], refs[k + i], refs[2 * k].at[i]) for i in range(k)]
    for copy in copies:
        copy.start()
    for copy in copies:
        copy.wait()


def written(name, *arrays):
    k = len(arrays)
    size = sum(a.size * a.dtype.itemsize for a in arrays)
    return pl.pallas_call(
        functools.partial(put_out, k),
        name=name,
        out_shape=[pltpu.HBM(a.shape, a.dtype) for a in arrays],
        in_specs=[IN_VMEM] * k,
        out_specs=[IN_HBM] * k,
        scratch_shapes=[pltpu.SemaphoreType.DMA((k,))],
        cost_estimate=pl.CostEstimate(flops=100 * size, bytes_accessed=size, transcendentals=0),
        compiler_params=pltpu.CompilerParams(has_side_effects=True, vmem_limit_bytes=VMEM_LIMIT),
    )(*arrays)


def patch(n, places, *refs):
    parts, outs, sem = refs[2:4], refs[4:6], refs[6]
    me = lax.axis_index("dp")
    far, core = (me // 2 + 2) % (n // 2), me % 2
    copies = []
    for i, of in enumerate((core, 1 - core)):
        first = 0
        for k, (t, s, size) in enumerate(places):
            copies.append(pltpu.make_async_copy(parts[i].at[pl.ds(first, size)], outs[t].at[of, far * 2 + of, pl.ds(s, size)], sem.at[i, k]))
            first += size
    for copy in copies:
        copy.start()
    for copy in copies:
        copy.wait()


IN_VMEM, IN_HBM = pl.BlockSpec(memory_space=pltpu.VMEM), pl.BlockSpec(memory_space=pltpu.HBM)


def solution(mesh):
    n = mesh.shape["dp"]
    chips = n // 2
    ring = [(2 * c + k, 2 * ((c + (1, chips - 1)[k]) % chips) + k) for c in range(chips) for k in range(2)]
    swap = [(d, d + 1 - 2 * (d % 2)) for d in range(n)]

    def step(*arrays):
        terms, weights, ms, vs = (arrays[i : i + 3] for i in (0, 3, 6, 9))
        layers = weights[0].shape[0]
        units = [one.shape[1] // ROWS for one in ms]
        cols = [one.shape[2] for one in ms]
        chunks, left = chunks_of(units)
        count = n * sum(one.size for one in ms)
        whole = [(layers, n, u, ROWS, c) for u, c in zip(units, cols)]
        part = [(layers, u, ROWS, c) for u, c in zip(units, cols)]
        over = (sum(chunks[i][2] for i in left), ROWS, cols[0])
        operands = (
            [t.reshape(s) for t, s in zip(terms, whole)]
            + [x.reshape(s) for x, s in zip(weights, whole)]
            + [x.reshape(s) for x, s in zip(ms, part)]
            + [x.reshape(s) for x, s in zip(vs, part)]
        )
        k = len(chunks)
        dma = pltpu.SemaphoreType.DMA
        outs = pl.pallas_call(
            functools.partial(kernel, n, count, chunks, left),
            name="step",
            out_shape=[pltpu.VMEM(s, BF16) for s in whole] + [pltpu.VMEM(s, F32) for s in part] * 2 + [pltpu.VMEM(over, BF16)],
            in_specs=[IN_HBM] * 12,
            out_specs=[IN_VMEM] * 10,
            scratch_shapes=[pltpu.VMEM((2, *s[1:]), BF16) for s in part]
            + [pltpu.VMEM(s, BF16) for s in part]
            + [pltpu.VMEM((ROWS, 128), F32), pltpu.VMEM((n, 1, 128), F32)]
            + [dma((3, 3)), dma((4, 2, k)), dma((3, 3)), dma((3, 2, k)), dma((2, 3)), dma((3, 3)), dma((n,)), dma((n,))],
            compiler_params=pltpu.CompilerParams(collective_id=0, has_side_effects=True, vmem_limit_bytes=VMEM_LIMIT),
        )(*[pltpu.with_memory_space_constraint(o, pltpu.HBM) for o in operands])
        over = lax.ppermute(outs[9], "dp", ring)
        outs = list(written("put_out", *outs[:9]))
        over = lax.optimization_barrier((over, outs[8]))[0]
        across = lax.ppermute(over, "dp", swap)
        outs[:2] = pl.pallas_call(
            functools.partial(patch, n, [chunks[i] for i in left]),
            name="patch",
            out_shape=[pltpu.HBM(o.shape, BF16) for o in outs[:2]],
            in_specs=[IN_HBM] * 2 + [IN_VMEM] * 2,
            out_specs=[IN_HBM] * 2,
            scratch_shapes=[dma((2, len(left)))],
            input_output_aliases={0: 0, 1: 1},
            compiler_params=pltpu.CompilerParams(has_side_effects=True, vmem_limit_bytes=VMEM_LIMIT),
        )(*outs[:2], *[pltpu.with_memory_space_constraint(o, pltpu.VMEM) for o in (over, across)])
        shapes = [x.shape for x in weights] + [x.shape for x in ms] * 2
        return tuple(o.reshape(s) for o, s in zip(outs, shapes))

    all_of, cut = P(None, None, None), P(None, "dp", None)
    return jax.shard_map(
        step,
        mesh=mesh,
        in_specs=(P(("rep", "dp"), None, None, None),) * 3 + (all_of,) * 3 + (cut,) * 6,
        out_specs=(P("rep", None, None),) * 3 + (P("rep", "dp", None),) * 6,
        check_vma=False,
    )
```

```python
import functools

import jax
import jax.numpy as jnp
from jax import lax
from jax.experimental import pallas as pl
from jax.experimental.pallas import tpu as pltpu
from jax.sharding import PartitionSpec as P

MESH = pl.DeviceIdType.MESH
ROWS = 16
VMEM_LIMIT = 8 * 2**20
F32, BF16 = jnp.float32, jnp.bfloat16
LAYERS = (0, 1)


def chunks_of(units):
    gate, up, down = units
    a, b = gate // 7, 3 * gate // 7
    head = [(0, 0, a), (0, a, b - a), (0, b, gate - b), (1, 0, up)]
    c = down - down // 10
    sums = head + [(2, 0, c), (2, c, down - c)]
    cuts = [k * down // 20 for k in (0, 14, 18, 20)]
    return sums, head + [(2, c, d - c) for c, d in zip(cuts, cuts[1:])], (1, 2, 3)


def kernel(n, count, sums, chunks, left, *refs):
    g, w, m_in, v_in = refs[0:3], refs[3:6], refs[6:9], refs[9:12]
    new, m, v = refs[12:15], refs[15:18], refs[18:21]
    piece = refs[21]
    own, old = refs[22:25], refs[25:28]
    total, squares = refs[28:30]
    (d2d_send, d2d_recv, ici_send, ici_recv, load_sem, state_sem, sq_send, sq_recv) = refs[30:]

    me = lax.axis_index("dp")
    chip, core = me // 2, me % 2
    chips = n // 2
    partner = chip * 2 + 1 - core
    down_, up_, far = (chip + chips - 1) % chips, (chip + 1) % chips, (chip + 2) % chips
    sides = (down_, up_)

    def at(c):
        return c * 2 + core

    def remote(src, dst, send, recv, to):
        return pltpu.make_async_remote_copy(src_ref=src, dst_ref=dst, send_sem=send, recv_sem=recv, device_id={"dp": to}, device_id_type=MESH)

    blocks = ((far, far), (up_, down_), (down_, up_), (chip, chip))
    target = ((down_, up_), (up_, down_), (down_, up_))

    def load(p, l, t):
        return pltpu.make_async_copy(g[t].at[l, at(blocks[p][l])], own[t].at[l], load_sem.at[l, t])

    def state():
        return [
            copy
            for t in range(3)
            for copy in (
                pltpu.make_async_copy(w[t].at[:, me], old[t], state_sem.at[0, t]),
                pltpu.make_async_copy(m_in[t], m[t], state_sem.at[1, t]),
                pltpu.make_async_copy(v_in[t], v[t], state_sem.at[2, t]),
            )
        ]

    for t in range(3):
        for l in LAYERS:
            load(0, l, t).start()

    barrier = pltpu.get_barrier_semaphore()
    for k in (partner, at(down_), at(up_)):
        pl.semaphore_signal(barrier, inc=1, device_id={"dp": k}, device_id_type=MESH)
    pl.semaphore_wait(barrier, 3)

    def handed(p, l, i):
        t, s, size = sums[i]
        there = blocks[p][l] * 2 + 1 - core
        part = (l, there, pl.ds(s, size))
        return remote(g[t].at[part], new[t].at[part], d2d_send.at[0, t], d2d_recv.at[p, l, i], partner)

    for p in range(4):
        for i in range(len(sums)):
            for l in LAYERS:
                handed(p, l, i).start()

    def inbox(j):
        return j * 2 + 1 - core

    def passed(p, l, i):
        t, s, size = sums[i]
        return remote(
            new[t].at[l, at(blocks[p][l]), pl.ds(s, size)],
            new[t].at[l, inbox(p), pl.ds(s, size)],
            ici_send.at[0, t],
            ici_recv.at[p, l, i],
            at(target[p][l]),
        )

    total[...] = jnp.zeros_like(total)

    def add(p, l, i):
        t, s, size = sums[i]
        block = at(blocks[p][l])

        @pl.loop(s, s + size)
        def _(r):
            x = own[t][l, r].astype(F32) + new[t][l, block, r].astype(F32)
            if p == 2:
                x = x + new[t][l, inbox(0), r].astype(F32)
            if p == 3:
                x = x + new[t][l, inbox(1), r].astype(F32) + new[t][l, inbox(2), r].astype(F32)
            x = x.astype(BF16)
            new[t][l, block, r] = x
            if p == 3:
                x = x.astype(F32)
                x = x * x
                parts = [x[:, k : k + 128] for k in range(0, x.shape[1], 128)]
                while len(parts) > 1:
                    parts = [a + b for a, b in zip(parts[::2], parts[1::2])] + ([parts[-1]] if len(parts) % 2 else [])
                total[...] += parts[0]

    for p in range(4):
        for i, (t, s, size) in enumerate(sums):
            for l in LAYERS:
                if s == 0:
                    load(p, l, t).wait()
                handed(p, l, i).wait_recv()
                if p == 2:
                    passed(0, l, i).wait_recv()
                if p == 3:
                    passed(1, l, i).wait_recv()
                    passed(2, l, i).wait_recv()
                add(p, l, i)
                if p < 3:
                    passed(p, l, i).start()
                    if s + size == g[t].shape[2]:
                        load(p + 1, l, t).start()
        if p == 2:
            for copy in state():
                copy.start()

    def sent(t, blocks, sem):
        part = new[t].at[:, pl.ds(0, blocks)]
        pltpu.make_async_copy(part, part, sem).wait()

    for t in range(3):
        sent(t, 4, d2d_send.at[0, t])
        sent(t, 3, ici_send.at[0, t])

    def told(k):
        return remote(squares.at[me], squares.at[me], sq_send.at[k], sq_recv.at[k], (me + k) % n)

    squares[me] = jnp.sum(total[...], axis=0, keepdims=True)
    for k in range(1, n):
        told(k).start()
    for copy in state():
        copy.wait()
    for k in range(1, n):
        told(k).wait_recv()
    everything = squares[0]
    for k in range(1, n):
        everything = everything + squares[k]
    everything = jnp.sum(everything, axis=(0, 1), keepdims=True)
    factor = jnp.minimum(1.0, 0.5 * lax.rsqrt(everything / count + 1e-30))

    def kind(q, last, i):
        return 0 if q < last else 2 if i in left else 1

    def spread(q, l, i):
        t, s, size = chunks[i]
        block = (chip, chip, sides[l])[q]
        part = (l, at(block), pl.ds(s, size))
        to = (sides[1 - l], sides[l], sides[1 - l])[q]
        return remote(new[t].at[part], new[t].at[part], ici_send.at[kind(q, 2, i), t], ici_recv.at[q, l, i], at(to))

    def came(q, l):
        return (sides[l], sides[1 - l], far)[q]

    def share(q, l, i):
        t, s, size = chunks[i]
        block = chip if q == 0 else came(q - 1, l)
        part = (l, at(block), pl.ds(s, size))
        arrived = d2d_recv.at[3, l, i] if q == 3 else d2d_recv.at[0, 0, t]
        return remote(new[t].at[part], new[t].at[part], d2d_send.at[kind(q, 3, i), t], arrived, partner)

    def keep(l, i):
        t, s, size = chunks[i]
        first = sum(chunks[k][2] for k in left if k < i)

        @pl.loop(0, size)
        def _(r):
            piece[first + r] = new[t][l, at(sides[l]), s + r]

    def passes(l, i, action):
        if i in left:
            pl.when(core != l)(action)
        else:
            action()

    for i, (t, s, size) in enumerate(chunks):
        for l in LAYERS:

            @pl.loop(s, s + size)
            def _(r, t=t, l=l):
                grad = new[t][l, me, r].astype(F32) * factor
                m1 = 0.9 * m[t][l, r] + 0.1 * grad
                v1 = 0.95 * v[t][l, r] + 0.05 * grad * grad
                w0 = old[t][l, r].astype(F32)
                step = m1 * lax.rsqrt(v1 + 1e-8) + 0.1 * w0
                new[t][l, me, r] = (w0 - 0.02 * step).astype(BF16)
                m[t][l, r] = m1
                v[t][l, r] = v1

            spread(0, l, i).start()
            share(0, l, i).start()
    for i in range(len(chunks)):
        for l in LAYERS:
            spread(1, l, i).start()
    for k in range(1, n):
        told(k).wait_send()
    for q in range(3):
        for i in range(len(chunks)):
            for l in LAYERS:

                def arrival(q=q, l=l, i=i):
                    spread(q, l, i).wait_recv()
                    share(q + 1, l, i).start()

                if q < 2:
                    spread(q, l, i).wait_recv()
                    if q == 0:
                        passes(l, i, lambda l=l, i=i: spread(2, l, i).start())
                    share(q + 1, l, i).start()
                    if q == 0 and i in left:
                        pl.when(core == l)(lambda l=l, i=i: keep(l, i))
                else:
                    passes(l, i, arrival)
        if q == 1:
            for t in range(3):
                sent(t, 2, ici_send.at[0, t])
    for t in range(3):
        sent(t, 3, d2d_recv.at[0, 0, t])
        sent(t, 3, d2d_send.at[0, t])
    for i in range(len(chunks)):
        for l in LAYERS:
            if i in left:
                pl.when(core == l)(lambda l=l, i=i: share(3, l, i).wait_recv())
            else:
                share(3, l, i).wait_recv()
    for t in range(3):
        units = sum(chunks[i][2] for i in left if chunks[i][0] == t)
        for part, sems in ((new[t].at[:, 0, pl.ds(0, new[t].shape[2] - units)], 1), (new[t].at[0, 0, pl.ds(0, units)], 2)):
            if part.shape[-3]:
                pltpu.make_async_copy(part, part, d2d_send.at[sems, t]).wait()
                pltpu.make_async_copy(part, part, ici_send.at[sems, t]).wait()


def put_out(k, *refs):
    copies = [pltpu.make_async_copy(refs[i], refs[k + i], refs[2 * k].at[i]) for i in range(k)]
    for copy in copies:
        copy.start()
    for copy in copies:
        copy.wait()


def written(name, *arrays):
    k = len(arrays)
    size = sum(a.size * a.dtype.itemsize for a in arrays)
    return pl.pallas_call(
        functools.partial(put_out, k),
        name=name,
        out_shape=[pltpu.HBM(a.shape, a.dtype) for a in arrays],
        in_specs=[IN_VMEM] * k,
        out_specs=[IN_HBM] * k,
        scratch_shapes=[pltpu.SemaphoreType.DMA((k,))],
        cost_estimate=pl.CostEstimate(flops=100 * size, bytes_accessed=size, transcendentals=0),
        compiler_params=pltpu.CompilerParams(has_side_effects=True, vmem_limit_bytes=VMEM_LIMIT),
    )(*arrays)


def patch(n, own, places, *refs):
    piece, outs, sem = refs[2], refs[3:5], refs[5]
    me = lax.axis_index("dp")
    far, core = (me // 2 + 2) % (n // 2), me % 2
    of = core if own else 1 - core
    copies, first = [], 0
    for k, (t, s, size) in enumerate(places):
        copies.append(pltpu.make_async_copy(piece.at[pl.ds(first, size)], outs[t].at[of, far * 2 + of, pl.ds(s, size)], sem.at[k]))
        first += size
    for copy in copies:
        copy.start()
    for copy in copies:
        copy.wait()


def patched(name, n, own, places, outs, piece):
    return pl.pallas_call(
        functools.partial(patch, n, own, places),
        name=name,
        out_shape=[pltpu.HBM(o.shape, BF16) for o in outs],
        in_specs=[IN_HBM] * 2 + [IN_VMEM],
        out_specs=[IN_HBM] * 2,
        scratch_shapes=[pltpu.SemaphoreType.DMA((len(places),))],
        input_output_aliases={0: 0, 1: 1},
        cost_estimate=pl.CostEstimate(flops=100 * piece.size, bytes_accessed=2 * piece.size, transcendentals=0),
        compiler_params=pltpu.CompilerParams(has_side_effects=True, vmem_limit_bytes=VMEM_LIMIT),
    )(*outs, pltpu.with_memory_space_constraint(piece, pltpu.VMEM))


IN_VMEM, IN_HBM = pl.BlockSpec(memory_space=pltpu.VMEM), pl.BlockSpec(memory_space=pltpu.HBM)


def solution(mesh):
    n = mesh.shape["dp"]
    chips = n // 2
    ring = [(2 * c + k, 2 * ((c + (1, chips - 1)[k]) % chips) + k) for c in range(chips) for k in range(2)]
    swap = [(d, d + 1 - 2 * (d % 2)) for d in range(n)]

    def step(*arrays):
        terms, weights, ms, vs = (arrays[i : i + 3] for i in (0, 3, 6, 9))
        layers = weights[0].shape[0]
        units = [one.shape[1] // ROWS for one in ms]
        cols = [one.shape[2] for one in ms]
        sums, chunks, left = chunks_of(units)
        count = n * sum(one.size for one in ms)
        whole = [(layers, n, u, ROWS, c) for u, c in zip(units, cols)]
        part = [(layers, u, ROWS, c) for u, c in zip(units, cols)]
        over = (sum(chunks[i][2] for i in left), ROWS, cols[0])
        operands = (
            [t.reshape(s) for t, s in zip(terms, whole)]
            + [x.reshape(s) for x, s in zip(weights, whole)]
            + [x.reshape(s) for x, s in zip(ms, part)]
            + [x.reshape(s) for x, s in zip(vs, part)]
        )
        k = max(len(sums), len(chunks))
        dma = pltpu.SemaphoreType.DMA
        outs = pl.pallas_call(
            functools.partial(kernel, n, count, sums, chunks, left),
            name="step",
            out_shape=[pltpu.VMEM(s, BF16) for s in whole] + [pltpu.VMEM(s, F32) for s in part] * 2 + [pltpu.VMEM(over, BF16)],
            in_specs=[IN_HBM] * 12,
            out_specs=[IN_VMEM] * 10,
            scratch_shapes=[pltpu.VMEM((2, *s[1:]), BF16) for s in part]
            + [pltpu.VMEM(s, BF16) for s in part]
            + [pltpu.VMEM((ROWS, 128), F32), pltpu.VMEM((n, 1, 128), F32)]
            + [dma((3, 3)), dma((4, 2, k)), dma((3, 3)), dma((3, 2, k)), dma((2, 3)), dma((3, 3)), dma((n,)), dma((n,))],
            compiler_params=pltpu.CompilerParams(collective_id=0, has_side_effects=True, vmem_limit_bytes=VMEM_LIMIT),
        )(*[pltpu.with_memory_space_constraint(o, pltpu.HBM) for o in operands])
        over = lax.ppermute(outs[9], "dp", ring)
        outs = list(written("put_out", *outs[:9]))
        over = lax.optimization_barrier((over, outs[8]))[0]
        across = lax.ppermute(over, "dp", swap)
        places = [chunks[i] for i in left]
        outs[:2] = patched("patch_own", n, True, places, outs[:2], over)
        outs[:2] = patched("patch_partner", n, False, places, outs[:2], across)
        shapes = [x.shape for x in weights] + [x.shape for x in ms] * 2
        return tuple(o.reshape(s) for o, s in zip(outs, shapes))

    all_of, cut = P(None, None, None), P(None, "dp", None)
    return jax.shard_map(
        step,
        mesh=mesh,
        in_specs=(P(("rep", "dp"), None, None, None),) * 3 + (all_of,) * 3 + (cut,) * 6,
        out_specs=(P("rep", None, None),) * 3 + (P("rep", "dp", None),) * 6,
        check_vma=False,
    )
```

```python
import functools

import jax
import jax.numpy as jnp
from jax import lax
from jax.experimental import pallas as pl
from jax.experimental.pallas import tpu as pltpu
from jax.sharding import PartitionSpec as P

MESH = pl.DeviceIdType.MESH
ROWS = 16
VMEM_LIMIT = 8 * 2**20
F32, BF16 = jnp.float32, jnp.bfloat16
LAYERS = (0, 1)


def chunks_of(units):
    gate, up, down = units
    a, b = gate // 7, 3 * gate // 7
    head = [(0, 0, a), (0, a, gate - a), (1, 0, up)]
    c = down - down // 10
    sums = head + [(2, 0, c), (2, c, down - c)]
    cuts = [k * down // 20 for k in (0, 14, 18, 20)]
    return sums, head + [(2, c, d - c) for c, d in zip(cuts, cuts[1:])], (1, 2)


def kernel(n, count, sums, chunks, left, *refs):
    g, w, m_in, v_in = refs[0:3], refs[3:6], refs[6:9], refs[9:12]
    new, m, v = refs[12:15], refs[15:18], refs[18:21]
    piece = refs[21]
    own, old = refs[22:25], refs[25:28]
    total, squares = refs[28:30]
    (d2d_send, d2d_recv, ici_send, ici_recv, load_sem, state_sem, sq_send, sq_recv) = refs[30:]

    me = lax.axis_index("dp")
    chip, core = me // 2, me % 2
    chips = n // 2
    partner = chip * 2 + 1 - core
    down_, up_, far = (chip + chips - 1) % chips, (chip + 1) % chips, (chip + 2) % chips
    sides = (down_, up_)

    def at(c):
        return c * 2 + core

    def remote(src, dst, send, recv, to):
        return pltpu.make_async_remote_copy(src_ref=src, dst_ref=dst, send_sem=send, recv_sem=recv, device_id={"dp": to}, device_id_type=MESH)

    blocks = ((far, far), (up_, down_), (down_, up_), (chip, chip))
    target = ((down_, up_), (up_, down_), (down_, up_))

    def load(p, l, t):
        return pltpu.make_async_copy(g[t].at[l, at(blocks[p][l])], own[t].at[l], load_sem.at[l, t])

    def state():
        return [
            copy
            for t in range(3)
            for copy in (
                pltpu.make_async_copy(w[t].at[:, me], old[t], state_sem.at[0, t]),
                pltpu.make_async_copy(m_in[t], m[t], state_sem.at[1, t]),
                pltpu.make_async_copy(v_in[t], v[t], state_sem.at[2, t]),
            )
        ]

    for t in range(3):
        for l in LAYERS:
            load(0, l, t).start()

    barrier = pltpu.get_barrier_semaphore()
    for k in (partner, at(down_), at(up_)):
        pl.semaphore_signal(barrier, inc=1, device_id={"dp": k}, device_id_type=MESH)
    pl.semaphore_wait(barrier, 3)

    def handed(p, l, i):
        t, s, size = sums[i]
        there = blocks[p][l] * 2 + 1 - core
        part = (l, there, pl.ds(s, size))
        return remote(g[t].at[part], new[t].at[part], d2d_send.at[0, t], d2d_recv.at[p, l, i], partner)

    for p in range(4):
        for i in range(len(sums)):
            for l in LAYERS:
                handed(p, l, i).start()

    def inbox(j):
        return j * 2 + 1 - core

    def passed(p, l, i):
        t, s, size = sums[i]
        return remote(
            new[t].at[l, at(blocks[p][l]), pl.ds(s, size)],
            new[t].at[l, inbox(p), pl.ds(s, size)],
            ici_send.at[0, t],
            ici_recv.at[p, l, i],
            at(target[p][l]),
        )

    total[...] = jnp.zeros_like(total)

    def add(p, l, i):
        t, s, size = sums[i]
        block = at(blocks[p][l])

        @pl.loop(s, s + size)
        def _(r):
            x = own[t][l, r].astype(F32) + new[t][l, block, r].astype(F32)
            if p == 2:
                x = x + new[t][l, inbox(0), r].astype(F32)
            if p == 3:
                x = x + new[t][l, inbox(1), r].astype(F32) + new[t][l, inbox(2), r].astype(F32)
            x = x.astype(BF16)
            new[t][l, block, r] = x
            if p == 3:
                x = x.astype(F32)
                x = x * x
                parts = [x[:, k : k + 128] for k in range(0, x.shape[1], 128)]
                while len(parts) > 1:
                    parts = [a + b for a, b in zip(parts[::2], parts[1::2])] + ([parts[-1]] if len(parts) % 2 else [])
                total[...] += parts[0]

    for p in range(4):
        for i, (t, s, size) in enumerate(sums):
            for l in LAYERS:
                if s == 0:
                    load(p, l, t).wait()
                handed(p, l, i).wait_recv()
                if p == 2:
                    passed(0, l, i).wait_recv()
                if p == 3:
                    passed(1, l, i).wait_recv()
                    passed(2, l, i).wait_recv()
                add(p, l, i)
                if p < 3:
                    passed(p, l, i).start()
                    if s + size == g[t].shape[2]:
                        load(p + 1, l, t).start()
        if p == 2:
            for copy in state():
                copy.start()

    def sent(t, blocks, sem):
        part = new[t].at[:, pl.ds(0, blocks)]
        pltpu.make_async_copy(part, part, sem).wait()

    for t in range(3):
        sent(t, 4, d2d_send.at[0, t])
        sent(t, 3, ici_send.at[0, t])

    def told(k):
        return remote(squares.at[me], squares.at[me], sq_send.at[k], sq_recv.at[k], (me + k) % n)

    squares[me] = jnp.sum(total[...], axis=0, keepdims=True)
    for k in range(1, n):
        told(k).start()
    for copy in state():
        copy.wait()
    for k in range(1, n):
        told(k).wait_recv()
    everything = squares[0]
    for k in range(1, n):
        everything = everything + squares[k]
    everything = jnp.sum(everything, axis=(0, 1), keepdims=True)
    factor = jnp.minimum(1.0, 0.5 * lax.rsqrt(everything / count + 1e-30))

    def kind(q, last, i):
        return 0 if q < last else 2 if i in left else 1

    def spread(q, l, i):
        t, s, size = chunks[i]
        block = (chip, chip, sides[l])[q]
        part = (l, at(block), pl.ds(s, size))
        to = (sides[1 - l], sides[l], sides[1 - l])[q]
        return remote(new[t].at[part], new[t].at[part], ici_send.at[kind(q, 2, i), t], ici_recv.at[q, l, i], at(to))

    def came(q, l):
        return (sides[l], sides[1 - l], far)[q]

    def share(q, l, i):
        t, s, size = chunks[i]
        block = chip if q == 0 else came(q - 1, l)
        part = (l, at(block), pl.ds(s, size))
        arrived = d2d_recv.at[3, l, i] if q == 3 else d2d_recv.at[0, 0, t]
        return remote(new[t].at[part], new[t].at[part], d2d_send.at[kind(q, 3, i), t], arrived, partner)

    def keep(l, i):
        t, s, size = chunks[i]
        first = sum(chunks[k][2] for k in left if k < i)

        @pl.loop(0, size)
        def _(r):
            piece[first + r] = new[t][l, at(sides[l]), s + r]

    def passes(l, i, action):
        if i in left:
            pl.when(core != l)(action)
        else:
            action()

    for i, (t, s, size) in enumerate(chunks):
        for l in LAYERS:

            @pl.loop(s, s + size)
            def _(r, t=t, l=l):
                grad = new[t][l, me, r].astype(F32) * factor
                m1 = 0.9 * m[t][l, r] + 0.1 * grad
                v1 = 0.95 * v[t][l, r] + 0.05 * grad * grad
                w0 = old[t][l, r].astype(F32)
                step = m1 * lax.rsqrt(v1 + 1e-8) + 0.1 * w0
                new[t][l, me, r] = (w0 - 0.02 * step).astype(BF16)
                m[t][l, r] = m1
                v[t][l, r] = v1

            spread(0, l, i).start()
            share(0, l, i).start()
    for i in range(len(chunks)):
        for l in LAYERS:
            spread(1, l, i).start()
    for k in range(1, n):
        told(k).wait_send()
    for q in range(3):
        for i in range(len(chunks)):
            for l in LAYERS:

                def arrival(q=q, l=l, i=i):
                    spread(q, l, i).wait_recv()
                    share(q + 1, l, i).start()

                if q < 2:
                    spread(q, l, i).wait_recv()
                    if q == 0:
                        passes(l, i, lambda l=l, i=i: spread(2, l, i).start())
                    share(q + 1, l, i).start()
                    if q == 0 and i in left:
                        pl.when(core == l)(lambda l=l, i=i: keep(l, i))
                else:
                    passes(l, i, arrival)
        if q == 1:
            for t in range(3):
                sent(t, 2, ici_send.at[0, t])
    for t in range(3):
        sent(t, 3, d2d_recv.at[0, 0, t])
        sent(t, 3, d2d_send.at[0, t])
    for i in range(len(chunks)):
        for l in LAYERS:
            if i in left:
                pl.when(core == l)(lambda l=l, i=i: share(3, l, i).wait_recv())
            else:
                share(3, l, i).wait_recv()
    for t in range(3):
        units = sum(chunks[i][2] for i in left if chunks[i][0] == t)
        for part, sems in ((new[t].at[:, 0, pl.ds(0, new[t].shape[2] - units)], 1), (new[t].at[0, 0, pl.ds(0, units)], 2)):
            if part.shape[-3]:
                pltpu.make_async_copy(part, part, d2d_send.at[sems, t]).wait()
                pltpu.make_async_copy(part, part, ici_send.at[sems, t]).wait()


def put_out(k, *refs):
    copies = [pltpu.make_async_copy(refs[i], refs[k + i], refs[2 * k].at[i]) for i in range(k)]
    for copy in copies:
        copy.start()
    for copy in copies:
        copy.wait()


def written(name, *arrays):
    k = len(arrays)
    size = sum(a.size * a.dtype.itemsize for a in arrays)
    return pl.pallas_call(
        functools.partial(put_out, k),
        name=name,
        out_shape=[pltpu.HBM(a.shape, a.dtype) for a in arrays],
        in_specs=[IN_VMEM] * k,
        out_specs=[IN_HBM] * k,
        scratch_shapes=[pltpu.SemaphoreType.DMA((k,))],
        cost_estimate=pl.CostEstimate(flops=100 * size, bytes_accessed=size, transcendentals=0),
        compiler_params=pltpu.CompilerParams(has_side_effects=True, vmem_limit_bytes=VMEM_LIMIT),
    )(*arrays)


def patch(n, own, places, *refs):
    piece, outs, sem = refs[2], refs[3:5], refs[5]
    me = lax.axis_index("dp")
    far, core = (me // 2 + 2) % (n // 2), me % 2
    of = core if own else 1 - core
    copies, first = [], 0
    for k, (t, s, size) in enumerate(places):
        copies.append(pltpu.make_async_copy(piece.at[pl.ds(first, size)], outs[t].at[of, far * 2 + of, pl.ds(s, size)], sem.at[k]))
        first += size
    for copy in copies:
        copy.start()
    for copy in copies:
        copy.wait()


def patched(name, n, own, places, outs, piece):
    return pl.pallas_call(
        functools.partial(patch, n, own, places),
        name=name,
        out_shape=[pltpu.HBM(o.shape, BF16) for o in outs],
        in_specs=[IN_HBM] * 2 + [IN_VMEM],
        out_specs=[IN_HBM] * 2,
        scratch_shapes=[pltpu.SemaphoreType.DMA((len(places),))],
        input_output_aliases={0: 0, 1: 1},
        cost_estimate=pl.CostEstimate(flops=100 * piece.size, bytes_accessed=2 * piece.size, transcendentals=0),
        compiler_params=pltpu.CompilerParams(has_side_effects=True, vmem_limit_bytes=VMEM_LIMIT),
    )(*outs, pltpu.with_memory_space_constraint(piece, pltpu.VMEM))


IN_VMEM, IN_HBM = pl.BlockSpec(memory_space=pltpu.VMEM), pl.BlockSpec(memory_space=pltpu.HBM)


def solution(mesh):
    n = mesh.shape["dp"]
    chips = n // 2
    ring = [(2 * c + k, 2 * ((c + (1, chips - 1)[k]) % chips) + k) for c in range(chips) for k in range(2)]
    swap = [(d, d + 1 - 2 * (d % 2)) for d in range(n)]

    def step(*arrays):
        terms, weights, ms, vs = (arrays[i : i + 3] for i in (0, 3, 6, 9))
        layers = weights[0].shape[0]
        units = [one.shape[1] // ROWS for one in ms]
        cols = [one.shape[2] for one in ms]
        sums, chunks, left = chunks_of(units)
        count = n * sum(one.size for one in ms)
        whole = [(layers, n, u, ROWS, c) for u, c in zip(units, cols)]
        part = [(layers, u, ROWS, c) for u, c in zip(units, cols)]
        over = (sum(chunks[i][2] for i in left), ROWS, cols[0])
        operands = (
            [t.reshape(s) for t, s in zip(terms, whole)]
            + [x.reshape(s) for x, s in zip(weights, whole)]
            + [x.reshape(s) for x, s in zip(ms, part)]
            + [x.reshape(s) for x, s in zip(vs, part)]
        )
        k = max(len(sums), len(chunks))
        dma = pltpu.SemaphoreType.DMA
        outs = pl.pallas_call(
            functools.partial(kernel, n, count, sums, chunks, left),
            name="step",
            out_shape=[pltpu.VMEM(s, BF16) for s in whole] + [pltpu.VMEM(s, F32) for s in part] * 2 + [pltpu.VMEM(over, BF16)],
            in_specs=[IN_HBM] * 12,
            out_specs=[IN_VMEM] * 10,
            scratch_shapes=[pltpu.VMEM((2, *s[1:]), BF16) for s in part]
            + [pltpu.VMEM(s, BF16) for s in part]
            + [pltpu.VMEM((ROWS, 128), F32), pltpu.VMEM((n, 1, 128), F32)]
            + [dma((3, 3)), dma((4, 2, k)), dma((3, 3)), dma((3, 2, k)), dma((2, 3)), dma((3, 3)), dma((n,)), dma((n,))],
            compiler_params=pltpu.CompilerParams(collective_id=0, has_side_effects=True, vmem_limit_bytes=VMEM_LIMIT),
        )(*[pltpu.with_memory_space_constraint(o, pltpu.HBM) for o in operands])
        over = lax.ppermute(outs[9], "dp", ring)
        outs = list(written("put_out", *outs[:9]))
        over = lax.optimization_barrier((over, outs[8]))[0]
        across = lax.ppermute(over, "dp", swap)
        places = [chunks[i] for i in left]
        outs[:2] = patched("patch_own", n, True, places, outs[:2], over)
        outs[:2] = patched("patch_partner", n, False, places, outs[:2], across)
        shapes = [x.shape for x in weights] + [x.shape for x in ms] * 2
        return tuple(o.reshape(s) for o, s in zip(outs, shapes))

    all_of, cut = P(None, None, None), P(None, "dp", None)
    return jax.shard_map(
        step,
        mesh=mesh,
        in_specs=(P(("rep", "dp"), None, None, None),) * 3 + (all_of,) * 3 + (cut,) * 6,
        out_specs=(P("rep", None, None),) * 3 + (P("rep", "dp", None),) * 6,
        check_vma=False,
    )
```

```python
import functools

import jax
import jax.numpy as jnp
from jax import lax
from jax.experimental import pallas as pl
from jax.experimental.pallas import tpu as pltpu
from jax.sharding import PartitionSpec as P

MESH = pl.DeviceIdType.MESH
ROWS = 16
VMEM_LIMIT = 8 * 2**20
F32, BF16 = jnp.float32, jnp.bfloat16
LAYERS = (0, 1)


def chunks_of(units):
    gate, up, down = units
    a, b = gate // 7, 3 * gate // 7
    head = [(0, 0, a), (0, a, gate - a), (1, 0, up)]
    c = down - down // 10
    sums = head + [(2, 0, c), (2, c, down - c)]
    cuts = [k * down // 20 for k in (0, 14, 18, 20)]
    return sums, head + [(2, c, d - c) for c, d in zip(cuts, cuts[1:])], (1, 2)


def kernel(n, count, sums, chunks, left, *refs):
    g, w, m_in, v_in = refs[0:3], refs[3:6], refs[6:9], refs[9:12]
    new, m, v = refs[12:15], refs[15:18], refs[18:21]
    piece = refs[21]
    own, old = refs[22:25], refs[25:28]
    total, squares = refs[28:30]
    (d2d_send, d2d_recv, ici_send, ici_recv, load_sem, state_sem, sq_send, sq_recv) = refs[30:]

    me = lax.axis_index("dp")
    chip, core = me // 2, me % 2
    chips = n // 2
    partner = chip * 2 + 1 - core
    down_, up_, far = (chip + chips - 1) % chips, (chip + 1) % chips, (chip + 2) % chips
    sides = (down_, up_)

    def at(c):
        return c * 2 + core

    def remote(src, dst, send, recv, to):
        return pltpu.make_async_remote_copy(src_ref=src, dst_ref=dst, send_sem=send, recv_sem=recv, device_id={"dp": to}, device_id_type=MESH)

    blocks = ((far, far), (up_, down_), (down_, up_), (chip, chip))
    target = ((down_, up_), (up_, down_), (down_, up_))

    def load(p, l, t):
        return pltpu.make_async_copy(g[t].at[l, at(blocks[p][l])], own[t].at[l], load_sem.at[l, t])

    def state():
        return [
            copy
            for t in range(3)
            for copy in (
                pltpu.make_async_copy(w[t].at[:, me], old[t], state_sem.at[0, t]),
                pltpu.make_async_copy(m_in[t], m[t], state_sem.at[1, t]),
                pltpu.make_async_copy(v_in[t], v[t], state_sem.at[2, t]),
            )
        ]

    for t in range(3):
        for l in LAYERS:
            load(0, l, t).start()

    barrier = pltpu.get_barrier_semaphore()
    for k in (partner, at(down_), at(up_)):
        pl.semaphore_signal(barrier, inc=1, device_id={"dp": k}, device_id_type=MESH)
    pl.semaphore_wait(barrier, 3)

    def handed(p, l, i):
        t, s, size = sums[i]
        there = blocks[p][l] * 2 + 1 - core
        part = (l, there, pl.ds(s, size))
        return remote(g[t].at[part], new[t].at[part], d2d_send.at[0, t], d2d_recv.at[p, l, i], partner)

    for p in range(4):
        for i in range(len(sums)):
            for l in LAYERS:
                handed(p, l, i).start()

    def inbox(j):
        return j * 2 + 1 - core

    def passed(p, l, i):
        t, s, size = sums[i]
        return remote(
            new[t].at[l, at(blocks[p][l]), pl.ds(s, size)],
            new[t].at[l, inbox(p), pl.ds(s, size)],
            ici_send.at[0, t],
            ici_recv.at[p, l, i],
            at(target[p][l]),
        )

    total[...] = jnp.zeros_like(total)

    def add(p, l, i):
        t, s, size = sums[i]
        block = at(blocks[p][l])

        @pl.loop(s, s + size)
        def _(r):
            x = own[t][l, r].astype(F32) + new[t][l, block, r].astype(F32)
            if p == 2:
                x = x + new[t][l, inbox(0), r].astype(F32)
            if p == 3:
                x = x + new[t][l, inbox(1), r].astype(F32) + new[t][l, inbox(2), r].astype(F32)
            x = x.astype(BF16)
            new[t][l, block, r] = x
            if p == 3:
                x = x.astype(F32)
                x = x * x
                parts = [x[:, k : k + 128] for k in range(0, x.shape[1], 128)]
                while len(parts) > 1:
                    parts = [a + b for a, b in zip(parts[::2], parts[1::2])] + ([parts[-1]] if len(parts) % 2 else [])
                total[...] += parts[0]

    for p in range(4):
        for i, (t, s, size) in enumerate(sums):
            for l in LAYERS:
                if s == 0:
                    load(p, l, t).wait()
                handed(p, l, i).wait_recv()
                if p == 2:
                    passed(0, l, i).wait_recv()
                if p == 3:
                    passed(1, l, i).wait_recv()
                    passed(2, l, i).wait_recv()
                add(p, l, i)
                if p < 3:
                    passed(p, l, i).start()
                    if s + size == g[t].shape[2]:
                        load(p + 1, l, t).start()
        if p == 2:
            for copy in state():
                copy.start()

    def sent(t, blocks, sem):
        part = new[t].at[:, pl.ds(0, blocks)]
        pltpu.make_async_copy(part, part, sem).wait()

    for t in range(3):
        sent(t, 4, d2d_send.at[0, t])
        sent(t, 3, ici_send.at[0, t])

    def told(k):
        return remote(squares.at[me], squares.at[me], sq_send.at[k], sq_recv.at[k], (me + k) % n)

    squares[me] = jnp.sum(total[...], axis=0, keepdims=True)
    for k in range(1, n):
        told(k).start()
    for copy in state():
        copy.wait()
    for k in range(1, n):
        told(k).wait_recv()
    everything = squares[0]
    for k in range(1, n):
        everything = everything + squares[k]
    everything = jnp.sum(everything, axis=(0, 1), keepdims=True)
    factor = jnp.minimum(1.0, 0.5 * lax.rsqrt(everything / count + 1e-30))

    def kind(q, last, i):
        return 0 if q < last else 2 if i in left else 1

    def spread(q, l, i):
        t, s, size = chunks[i]
        block = (chip, chip, sides[l])[q]
        part = (l, at(block), pl.ds(s, size))
        to = (sides[1 - l], sides[l], sides[1 - l])[q]
        return remote(new[t].at[part], new[t].at[part], ici_send.at[kind(q, 2, i), t], ici_recv.at[q, l, i], at(to))

    def came(q, l):
        return (sides[l], sides[1 - l], far)[q]

    def share(q, l, i):
        t, s, size = chunks[i]
        block = chip if q == 0 else came(q - 1, l)
        part = (l, at(block), pl.ds(s, size))
        arrived = d2d_recv.at[3, l, i] if q == 3 else d2d_recv.at[0, 0, t]
        return remote(new[t].at[part], new[t].at[part], d2d_send.at[kind(q, 3, i), t], arrived, partner)

    def keep(l, i):
        t, s, size = chunks[i]
        first = sum(chunks[k][2] for k in left if k < i)

        @pl.loop(0, size)
        def _(r):
            piece[first + r] = new[t][l, at(sides[l]), s + r]

    def passes(l, i, action):
        if i in left:
            pl.when(core == l)(action)
        else:
            action()

    for i, (t, s, size) in enumerate(chunks):
        for l in LAYERS:

            @pl.loop(s, s + size)
            def _(r, t=t, l=l):
                grad = new[t][l, me, r].astype(F32) * factor
                m1 = 0.9 * m[t][l, r] + 0.1 * grad
                v1 = 0.95 * v[t][l, r] + 0.05 * grad * grad
                w0 = old[t][l, r].astype(F32)
                step = m1 * lax.rsqrt(v1 + 1e-8) + 0.1 * w0
                new[t][l, me, r] = (w0 - 0.02 * step).astype(BF16)
                m[t][l, r] = m1
                v[t][l, r] = v1

            spread(0, l, i).start()
            share(0, l, i).start()
    for i in range(len(chunks)):
        for l in LAYERS:
            spread(1, l, i).start()
    for k in range(1, n):
        told(k).wait_send()
    for q in range(3):
        for i in range(len(chunks)):
            for l in LAYERS:

                def arrival(q=q, l=l, i=i):
                    spread(q, l, i).wait_recv()
                    share(q + 1, l, i).start()

                if q < 2:
                    spread(q, l, i).wait_recv()
                    if q == 0:
                        passes(l, i, lambda l=l, i=i: spread(2, l, i).start())
                    share(q + 1, l, i).start()
                    if q == 0 and i in left:
                        pl.when(core != l)(lambda l=l, i=i: keep(l, i))
                else:
                    passes(l, i, arrival)
        if q == 1:
            for t in range(3):
                sent(t, 2, ici_send.at[0, t])
    for t in range(3):
        sent(t, 3, d2d_recv.at[0, 0, t])
        sent(t, 3, d2d_send.at[0, t])
    for i in range(len(chunks)):
        for l in LAYERS:
            if i in left:
                pl.when(core != l)(lambda l=l, i=i: share(3, l, i).wait_recv())
            else:
                share(3, l, i).wait_recv()
    for t in range(3):
        units = sum(chunks[i][2] for i in left if chunks[i][0] == t)
        for part, sems in ((new[t].at[:, 0, pl.ds(0, new[t].shape[2] - units)], 1), (new[t].at[0, 0, pl.ds(0, units)], 2)):
            if part.shape[-3]:
                pltpu.make_async_copy(part, part, d2d_send.at[sems, t]).wait()
                pltpu.make_async_copy(part, part, ici_send.at[sems, t]).wait()


def put_out(k, *refs):
    copies = [pltpu.make_async_copy(refs[i], refs[k + i], refs[2 * k].at[i]) for i in range(k)]
    for copy in copies:
        copy.start()
    for copy in copies:
        copy.wait()


def written(name, *arrays):
    k = len(arrays)
    size = sum(a.size * a.dtype.itemsize for a in arrays)
    return pl.pallas_call(
        functools.partial(put_out, k),
        name=name,
        out_shape=[pltpu.HBM(a.shape, a.dtype) for a in arrays],
        in_specs=[IN_VMEM] * k,
        out_specs=[IN_HBM] * k,
        scratch_shapes=[pltpu.SemaphoreType.DMA((k,))],
        cost_estimate=pl.CostEstimate(flops=100 * size, bytes_accessed=size, transcendentals=0),
        compiler_params=pltpu.CompilerParams(has_side_effects=True, vmem_limit_bytes=VMEM_LIMIT),
    )(*arrays)


def patch(n, own, places, *refs):
    piece, outs, sem = refs[2], refs[3:5], refs[5]
    me = lax.axis_index("dp")
    far, core = (me // 2 + 2) % (n // 2), me % 2
    of = core if own else 1 - core
    copies, first = [], 0
    for k, (t, s, size) in enumerate(places):
        copies.append(pltpu.make_async_copy(piece.at[pl.ds(first, size)], outs[t].at[1 - of, far * 2 + of, pl.ds(s, size)], sem.at[k]))
        first += size
    for copy in copies:
        copy.start()
    for copy in copies:
        copy.wait()


def patched(name, n, own, places, outs, piece):
    return pl.pallas_call(
        functools.partial(patch, n, own, places),
        name=name,
        out_shape=[pltpu.HBM(o.shape, BF16) for o in outs],
        in_specs=[IN_HBM] * 2 + [IN_VMEM],
        out_specs=[IN_HBM] * 2,
        scratch_shapes=[pltpu.SemaphoreType.DMA((len(places),))],
        input_output_aliases={0: 0, 1: 1},
        cost_estimate=pl.CostEstimate(flops=100 * piece.size, bytes_accessed=2 * piece.size, transcendentals=0),
        compiler_params=pltpu.CompilerParams(has_side_effects=True, vmem_limit_bytes=VMEM_LIMIT),
    )(*outs, pltpu.with_memory_space_constraint(piece, pltpu.VMEM))


IN_VMEM, IN_HBM = pl.BlockSpec(memory_space=pltpu.VMEM), pl.BlockSpec(memory_space=pltpu.HBM)


def solution(mesh):
    n = mesh.shape["dp"]
    chips = n // 2
    ring = [(2 * c + k, 2 * ((c + (chips - 1, 1)[k]) % chips) + k) for c in range(chips) for k in range(2)]
    swap = [(d, d + 1 - 2 * (d % 2)) for d in range(n)]

    def step(*arrays):
        terms, weights, ms, vs = (arrays[i : i + 3] for i in (0, 3, 6, 9))
        layers = weights[0].shape[0]
        units = [one.shape[1] // ROWS for one in ms]
        cols = [one.shape[2] for one in ms]
        sums, chunks, left = chunks_of(units)
        count = n * sum(one.size for one in ms)
        whole = [(layers, n, u, ROWS, c) for u, c in zip(units, cols)]
        part = [(layers, u, ROWS, c) for u, c in zip(units, cols)]
        over = (sum(chunks[i][2] for i in left), ROWS, cols[0])
        operands = (
            [t.reshape(s) for t, s in zip(terms, whole)]
            + [x.reshape(s) for x, s in zip(weights, whole)]
            + [x.reshape(s) for x, s in zip(ms, part)]
            + [x.reshape(s) for x, s in zip(vs, part)]
        )
        k = max(len(sums), len(chunks))
        dma = pltpu.SemaphoreType.DMA
        outs = pl.pallas_call(
            functools.partial(kernel, n, count, sums, chunks, left),
            name="step",
            out_shape=[pltpu.VMEM(s, BF16) for s in whole] + [pltpu.VMEM(s, F32) for s in part] * 2 + [pltpu.VMEM(over, BF16)],
            in_specs=[IN_HBM] * 12,
            out_specs=[IN_VMEM] * 10,
            scratch_shapes=[pltpu.VMEM((2, *s[1:]), BF16) for s in part]
            + [pltpu.VMEM(s, BF16) for s in part]
            + [pltpu.VMEM((ROWS, 128), F32), pltpu.VMEM((n, 1, 128), F32)]
            + [dma((3, 3)), dma((4, 2, k)), dma((3, 3)), dma((3, 2, k)), dma((2, 3)), dma((3, 3)), dma((n,)), dma((n,))],
            compiler_params=pltpu.CompilerParams(collective_id=0, has_side_effects=True, vmem_limit_bytes=VMEM_LIMIT),
        )(*[pltpu.with_memory_space_constraint(o, pltpu.HBM) for o in operands])
        over = lax.ppermute(outs[9], "dp", ring)
        outs = list(written("put_out", *outs[:9]))
        over = lax.optimization_barrier((over, outs[8]))[0]
        across = lax.ppermute(over, "dp", swap)
        places = [chunks[i] for i in left]
        outs[:2] = patched("patch_own", n, True, places, outs[:2], over)
        outs[:2] = patched("patch_partner", n, False, places, outs[:2], across)
        shapes = [x.shape for x in weights] + [x.shape for x in ms] * 2
        return tuple(o.reshape(s) for o, s in zip(outs, shapes))

    all_of, cut = P(None, None, None), P(None, "dp", None)
    return jax.shard_map(
        step,
        mesh=mesh,
        in_specs=(P(("rep", "dp"), None, None, None),) * 3 + (all_of,) * 3 + (cut,) * 6,
        out_specs=(P("rep", None, None),) * 3 + (P("rep", "dp", None),) * 6,
        check_vma=False,
    )
```

```python
import functools

import jax
import jax.numpy as jnp
from jax import lax
from jax.experimental import pallas as pl
from jax.experimental.pallas import tpu as pltpu
from jax.sharding import PartitionSpec as P

MESH = pl.DeviceIdType.MESH
ROWS = 16
VMEM_LIMIT = 8 * 2**20
F32, BF16 = jnp.float32, jnp.bfloat16
LAYERS = (0, 1)


def chunks_of(units):
    gate, up, down = units
    a, b = gate // 7, 3 * gate // 7
    head = [(0, 0, a), (0, a, gate - a), (1, 0, up)]
    c = down - down // 10
    sums = head + [(2, 0, c), (2, c, down - c)]
    cuts = [k * down // 20 for k in (0, 15, 19, 20)]
    return sums, head + [(2, c, d - c) for c, d in zip(cuts, cuts[1:])], (1, 2)


def kernel(n, count, sums, chunks, left, *refs):
    g, w, m_in, v_in = refs[0:3], refs[3:6], refs[6:9], refs[9:12]
    new, m, v = refs[12:15], refs[15:18], refs[18:21]
    piece = refs[21]
    own, old = refs[22:25], refs[25:28]
    total, squares = refs[28:30]
    (d2d_send, d2d_recv, ici_send, ici_recv, load_sem, state_sem, sq_send, sq_recv) = refs[30:]

    me = lax.axis_index("dp")
    chip, core = me // 2, me % 2
    chips = n // 2
    partner = chip * 2 + 1 - core
    down_, up_, far = (chip + chips - 1) % chips, (chip + 1) % chips, (chip + 2) % chips
    sides = (down_, up_)

    def at(c):
        return c * 2 + core

    def remote(src, dst, send, recv, to):
        return pltpu.make_async_remote_copy(src_ref=src, dst_ref=dst, send_sem=send, recv_sem=recv, device_id={"dp": to}, device_id_type=MESH)

    blocks = ((far, far), (up_, down_), (down_, up_), (chip, chip))
    target = ((down_, up_), (up_, down_), (down_, up_))

    def load(p, l, t):
        return pltpu.make_async_copy(g[t].at[l, at(blocks[p][l])], own[t].at[l], load_sem.at[l, t])

    def state():
        return [
            copy
            for t in range(3)
            for copy in (
                pltpu.make_async_copy(w[t].at[:, me], old[t], state_sem.at[0, t]),
                pltpu.make_async_copy(m_in[t], m[t], state_sem.at[1, t]),
                pltpu.make_async_copy(v_in[t], v[t], state_sem.at[2, t]),
            )
        ]

    for t in range(3):
        for l in LAYERS:
            load(0, l, t).start()

    barrier = pltpu.get_barrier_semaphore()
    for k in (partner, at(down_), at(up_)):
        pl.semaphore_signal(barrier, inc=1, device_id={"dp": k}, device_id_type=MESH)
    pl.semaphore_wait(barrier, 3)

    def handed(p, l, i):
        t, s, size = sums[i]
        there = blocks[p][l] * 2 + 1 - core
        part = (l, there, pl.ds(s, size))
        return remote(g[t].at[part], new[t].at[part], d2d_send.at[0, t], d2d_recv.at[p, l, i], partner)

    for p in range(4):
        for i in range(len(sums)):
            for l in LAYERS:
                handed(p, l, i).start()

    def inbox(j):
        return j * 2 + 1 - core

    def passed(p, l, i):
        t, s, size = sums[i]
        return remote(
            new[t].at[l, at(blocks[p][l]), pl.ds(s, size)],
            new[t].at[l, inbox(p), pl.ds(s, size)],
            ici_send.at[0, t],
            ici_recv.at[p, l, i],
            at(target[p][l]),
        )

    total[...] = jnp.zeros_like(total)

    def add(p, l, i):
        t, s, size = sums[i]
        block = at(blocks[p][l])

        @pl.loop(s, s + size)
        def _(r):
            x = own[t][l, r].astype(F32) + new[t][l, block, r].astype(F32)
            if p == 2:
                x = x + new[t][l, inbox(0), r].astype(F32)
            if p == 3:
                x = x + new[t][l, inbox(1), r].astype(F32) + new[t][l, inbox(2), r].astype(F32)
            x = x.astype(BF16)
            new[t][l, block, r] = x
            if p == 3:
                x = x.astype(F32)
                x = x * x
                parts = [x[:, k : k + 128] for k in range(0, x.shape[1], 128)]
                while len(parts) > 1:
                    parts = [a + b for a, b in zip(parts[::2], parts[1::2])] + ([parts[-1]] if len(parts) % 2 else [])
                total[...] += parts[0]

    for p in range(4):
        for i, (t, s, size) in enumerate(sums):
            for l in LAYERS:
                if s == 0:
                    load(p, l, t).wait()
                handed(p, l, i).wait_recv()
                if p == 2:
                    passed(0, l, i).wait_recv()
                if p == 3:
                    passed(1, l, i).wait_recv()
                    passed(2, l, i).wait_recv()
                add(p, l, i)
                if p < 3:
                    passed(p, l, i).start()
                    if s + size == g[t].shape[2]:
                        load(p + 1, l, t).start()
        if p == 2:
            for copy in state():
                copy.start()

    def sent(t, blocks, sem):
        part = new[t].at[:, pl.ds(0, blocks)]
        pltpu.make_async_copy(part, part, sem).wait()

    for t in range(3):
        sent(t, 4, d2d_send.at[0, t])
        sent(t, 3, ici_send.at[0, t])

    def told(k):
        return remote(squares.at[me], squares.at[me], sq_send.at[k], sq_recv.at[k], (me + k) % n)

    squares[me] = jnp.sum(total[...], axis=0, keepdims=True)
    for k in sorted(range(1, n), key=lambda k: -min(k, n - k)):
        told(k).start()
    for copy in state():
        copy.wait()
    for k in range(1, n):
        told(k).wait_recv()
    everything = squares[0]
    for k in range(1, n):
        everything = everything + squares[k]
    everything = jnp.sum(everything, axis=(0, 1), keepdims=True)
    factor = jnp.minimum(1.0, 0.5 * lax.rsqrt(everything / count + 1e-30))

    def kind(q, last, i):
        return 0 if q < last else 2 if i in left else 1

    def spread(q, l, i):
        t, s, size = chunks[i]
        block = (chip, chip, sides[l])[q]
        part = (l, at(block), pl.ds(s, size))
        to = (sides[1 - l], sides[l], sides[1 - l])[q]
        return remote(new[t].at[part], new[t].at[part], ici_send.at[kind(q, 2, i), t], ici_recv.at[q, l, i], at(to))

    def came(q, l):
        return (sides[l], sides[1 - l], far)[q]

    def share(q, l, i):
        t, s, size = chunks[i]
        block = chip if q == 0 else came(q - 1, l)
        part = (l, at(block), pl.ds(s, size))
        arrived = d2d_recv.at[3, l, i] if q == 3 else d2d_recv.at[0, 0, t]
        return remote(new[t].at[part], new[t].at[part], d2d_send.at[kind(q, 3, i), t], arrived, partner)

    def keep(l, i):
        t, s, size = chunks[i]
        first = sum(chunks[k][2] for k in left if k < i)

        @pl.loop(0, size)
        def _(r):
            piece[first + r] = new[t][l, at(sides[l]), s + r]

    def passes(l, i, action):
        if i in left:
            pl.when(core == l)(action)
        else:
            action()

    for i, (t, s, size) in enumerate(chunks):
        for l in LAYERS:

            @pl.loop(s, s + size)
            def _(r, t=t, l=l):
                grad = new[t][l, me, r].astype(F32) * factor
                m1 = 0.9 * m[t][l, r] + 0.1 * grad
                v1 = 0.95 * v[t][l, r] + 0.05 * grad * grad
                w0 = old[t][l, r].astype(F32)
                step = m1 * lax.rsqrt(v1 + 1e-8) + 0.1 * w0
                new[t][l, me, r] = (w0 - 0.02 * step).astype(BF16)
                m[t][l, r] = m1
                v[t][l, r] = v1

            spread(0, l, i).start()
            share(0, l, i).start()
    for i in range(len(chunks)):
        for l in LAYERS:
            spread(1, l, i).start()
    for k in range(1, n):
        told(k).wait_send()
    for q in range(3):
        for i in range(len(chunks)):
            for l in LAYERS:

                def arrival(q=q, l=l, i=i):
                    spread(q, l, i).wait_recv()
                    share(q + 1, l, i).start()

                if q < 2:
                    spread(q, l, i).wait_recv()
                    if q == 0:
                        passes(l, i, lambda l=l, i=i: spread(2, l, i).start())
                    share(q + 1, l, i).start()
                    if q == 0 and i in left:
                        pl.when(core != l)(lambda l=l, i=i: keep(l, i))
                else:
                    passes(l, i, arrival)
        if q == 1:
            for t in range(3):
                sent(t, 2, ici_send.at[0, t])
    for t in range(3):
        sent(t, 3, d2d_recv.at[0, 0, t])
        sent(t, 3, d2d_send.at[0, t])
    for i in range(len(chunks)):
        for l in LAYERS:
            if i in left:
                pl.when(core != l)(lambda l=l, i=i: share(3, l, i).wait_recv())
            else:
                share(3, l, i).wait_recv()
    for t in range(3):
        units = sum(chunks[i][2] for i in left if chunks[i][0] == t)
        for part, sems in ((new[t].at[:, 0, pl.ds(0, new[t].shape[2] - units)], 1), (new[t].at[0, 0, pl.ds(0, units)], 2)):
            if part.shape[-3]:
                pltpu.make_async_copy(part, part, d2d_send.at[sems, t]).wait()
                pltpu.make_async_copy(part, part, ici_send.at[sems, t]).wait()


def put_out(k, *refs):
    copies = [pltpu.make_async_copy(refs[i], refs[k + i], refs[2 * k].at[i]) for i in range(k)]
    for copy in copies:
        copy.start()
    for copy in copies:
        copy.wait()


def written(name, *arrays):
    k = len(arrays)
    size = sum(a.size * a.dtype.itemsize for a in arrays)
    return pl.pallas_call(
        functools.partial(put_out, k),
        name=name,
        out_shape=[pltpu.HBM(a.shape, a.dtype) for a in arrays],
        in_specs=[IN_VMEM] * k,
        out_specs=[IN_HBM] * k,
        scratch_shapes=[pltpu.SemaphoreType.DMA((k,))],
        cost_estimate=pl.CostEstimate(flops=100 * size, bytes_accessed=size, transcendentals=0),
        compiler_params=pltpu.CompilerParams(has_side_effects=True, vmem_limit_bytes=VMEM_LIMIT),
    )(*arrays)


def patch(n, own, places, *refs):
    piece, outs, sem = refs[2], refs[3:5], refs[5]
    me = lax.axis_index("dp")
    far, core = (me // 2 + 2) % (n // 2), me % 2
    of = core if own else 1 - core
    copies, first = [], 0
    for k, (t, s, size) in enumerate(places):
        copies.append(pltpu.make_async_copy(piece.at[pl.ds(first, size)], outs[t].at[1 - of, far * 2 + of, pl.ds(s, size)], sem.at[k]))
        first += size
    for copy in copies:
        copy.start()
    for copy in copies:
        copy.wait()


def patched(name, n, own, places, outs, piece):
    return pl.pallas_call(
        functools.partial(patch, n, own, places),
        name=name,
        out_shape=[pltpu.HBM(o.shape, BF16) for o in outs],
        in_specs=[IN_HBM] * 2 + [IN_VMEM],
        out_specs=[IN_HBM] * 2,
        scratch_shapes=[pltpu.SemaphoreType.DMA((len(places),))],
        input_output_aliases={0: 0, 1: 1},
        cost_estimate=pl.CostEstimate(flops=100 * piece.size, bytes_accessed=2 * piece.size, transcendentals=0),
        compiler_params=pltpu.CompilerParams(has_side_effects=True, vmem_limit_bytes=VMEM_LIMIT),
    )(*outs, pltpu.with_memory_space_constraint(piece, pltpu.VMEM))


IN_VMEM, IN_HBM = pl.BlockSpec(memory_space=pltpu.VMEM), pl.BlockSpec(memory_space=pltpu.HBM)


def solution(mesh):
    n = mesh.shape["dp"]
    chips = n // 2
    ring = [(2 * c + k, 2 * ((c + (chips - 1, 1)[k]) % chips) + k) for c in range(chips) for k in range(2)]
    swap = [(d, d + 1 - 2 * (d % 2)) for d in range(n)]

    def step(*arrays):
        terms, weights, ms, vs = (arrays[i : i + 3] for i in (0, 3, 6, 9))
        layers = weights[0].shape[0]
        units = [one.shape[1] // ROWS for one in ms]
        cols = [one.shape[2] for one in ms]
        sums, chunks, left = chunks_of(units)
        count = n * sum(one.size for one in ms)
        whole = [(layers, n, u, ROWS, c) for u, c in zip(units, cols)]
        part = [(layers, u, ROWS, c) for u, c in zip(units, cols)]
        over = (sum(chunks[i][2] for i in left), ROWS, cols[0])
        operands = (
            [t.reshape(s) for t, s in zip(terms, whole)]
            + [x.reshape(s) for x, s in zip(weights, whole)]
            + [x.reshape(s) for x, s in zip(ms, part)]
            + [x.reshape(s) for x, s in zip(vs, part)]
        )
        k = max(len(sums), len(chunks))
        dma = pltpu.SemaphoreType.DMA
        outs = pl.pallas_call(
            functools.partial(kernel, n, count, sums, chunks, left),
            name="step",
            out_shape=[pltpu.VMEM(s, BF16) for s in whole] + [pltpu.VMEM(s, F32) for s in part] * 2 + [pltpu.VMEM(over, BF16)],
            in_specs=[IN_HBM] * 12,
            out_specs=[IN_VMEM] * 10,
            scratch_shapes=[pltpu.VMEM((2, *s[1:]), BF16) for s in part]
            + [pltpu.VMEM(s, BF16) for s in part]
            + [pltpu.VMEM((ROWS, 128), F32), pltpu.VMEM((n, 1, 128), F32)]
            + [dma((3, 3)), dma((4, 2, k)), dma((3, 3)), dma((3, 2, k)), dma((2, 3)), dma((3, 3)), dma((n,)), dma((n,))],
            compiler_params=pltpu.CompilerParams(collective_id=0, has_side_effects=True, vmem_limit_bytes=VMEM_LIMIT),
        )(*[pltpu.with_memory_space_constraint(o, pltpu.HBM) for o in operands])
        over = lax.ppermute(outs[9], "dp", ring)
        outs = list(written("put_out", *outs[:9]))
        over = lax.optimization_barrier((over, outs[8]))[0]
        across = lax.ppermute(over, "dp", swap)
        places = [chunks[i] for i in left]
        outs[:2] = patched("patch_own", n, True, places, outs[:2], over)
        outs[:2] = patched("patch_partner", n, False, places, outs[:2], across)
        shapes = [x.shape for x in weights] + [x.shape for x in ms] * 2
        return tuple(o.reshape(s) for o, s in zip(outs, shapes))

    all_of, cut = P(None, None, None), P(None, "dp", None)
    return jax.shard_map(
        step,
        mesh=mesh,
        in_specs=(P(("rep", "dp"), None, None, None),) * 3 + (all_of,) * 3 + (cut,) * 6,
        out_specs=(P("rep", None, None),) * 3 + (P("rep", "dp", None),) * 6,
        check_vma=False,
    )
```

```python
import functools

import jax
import jax.numpy as jnp
from jax import lax
from jax.experimental import pallas as pl
from jax.experimental.pallas import tpu as pltpu
from jax.sharding import PartitionSpec as P

MESH = pl.DeviceIdType.MESH
ROWS = 16
VMEM_LIMIT = 8 * 2**20
F32, BF16 = jnp.float32, jnp.bfloat16
LAYERS = (0, 1)


def chunks_of(units):
    gate, up, down = units
    a, b = gate // 7, 3 * gate // 7
    head = [(0, 0, a), (0, a, gate - a), (1, 0, up)]
    c = down - down // 10
    sums = head + [(2, 0, c), (2, c, down - c)]
    cuts = [k * down // 20 for k in (0, 15, 19, 20)]
    return sums, head + [(2, c, d - c) for c, d in zip(cuts, cuts[1:])], (0, 1, 2)


def kernel(n, count, sums, chunks, left, *refs):
    g, w, m_in, v_in = refs[0:3], refs[3:6], refs[6:9], refs[9:12]
    new, m, v = refs[12:15], refs[15:18], refs[18:21]
    piece = refs[21]
    own, old = refs[22:25], refs[25:28]
    total, squares = refs[28:30]
    (d2d_send, d2d_recv, ici_send, ici_recv, load_sem, state_sem, sq_send, sq_recv) = refs[30:]

    me = lax.axis_index("dp")
    chip, core = me // 2, me % 2
    chips = n // 2
    partner = chip * 2 + 1 - core
    down_, up_, far = (chip + chips - 1) % chips, (chip + 1) % chips, (chip + 2) % chips
    sides = (down_, up_)

    def at(c):
        return c * 2 + core

    def remote(src, dst, send, recv, to):
        return pltpu.make_async_remote_copy(src_ref=src, dst_ref=dst, send_sem=send, recv_sem=recv, device_id={"dp": to}, device_id_type=MESH)

    blocks = ((far, far), (up_, down_), (down_, up_), (chip, chip))
    target = ((down_, up_), (up_, down_), (down_, up_))

    def load(p, l, t):
        return pltpu.make_async_copy(g[t].at[l, at(blocks[p][l])], own[t].at[l], load_sem.at[l, t])

    def state():
        return [
            copy
            for t in range(3)
            for copy in (
                pltpu.make_async_copy(w[t].at[:, me], old[t], state_sem.at[0, t]),
                pltpu.make_async_copy(m_in[t], m[t], state_sem.at[1, t]),
                pltpu.make_async_copy(v_in[t], v[t], state_sem.at[2, t]),
            )
        ]

    for t in range(3):
        for l in LAYERS:
            load(0, l, t).start()

    barrier = pltpu.get_barrier_semaphore()
    for k in (partner, at(down_), at(up_)):
        pl.semaphore_signal(barrier, inc=1, device_id={"dp": k}, device_id_type=MESH)
    pl.semaphore_wait(barrier, 3)

    def handed(p, l, i):
        t, s, size = sums[i]
        there = blocks[p][l] * 2 + 1 - core
        part = (l, there, pl.ds(s, size))
        return remote(g[t].at[part], new[t].at[part], d2d_send.at[0, t], d2d_recv.at[p, l, i], partner)

    for p in range(4):
        for i in range(len(sums)):
            for l in LAYERS:
                handed(p, l, i).start()

    def inbox(j):
        return j * 2 + 1 - core

    def passed(p, l, i):
        t, s, size = sums[i]
        return remote(
            new[t].at[l, at(blocks[p][l]), pl.ds(s, size)],
            new[t].at[l, inbox(p), pl.ds(s, size)],
            ici_send.at[0, t],
            ici_recv.at[p, l, i],
            at(target[p][l]),
        )

    total[...] = jnp.zeros_like(total)

    def add(p, l, i):
        t, s, size = sums[i]
        block = at(blocks[p][l])

        @pl.loop(s, s + size)
        def _(r):
            x = own[t][l, r].astype(F32) + new[t][l, block, r].astype(F32)
            if p == 2:
                x = x + new[t][l, inbox(0), r].astype(F32)
            if p == 3:
                x = x + new[t][l, inbox(1), r].astype(F32) + new[t][l, inbox(2), r].astype(F32)
            x = x.astype(BF16)
            new[t][l, block, r] = x
            if p == 3:
                x = x.astype(F32)
                x = x * x
                parts = [x[:, k : k + 128] for k in range(0, x.shape[1], 128)]
                while len(parts) > 1:
                    parts = [a + b for a, b in zip(parts[::2], parts[1::2])] + ([parts[-1]] if len(parts) % 2 else [])
                total[...] += parts[0]

    for p in range(4):
        for i, (t, s, size) in enumerate(sums):
            for l in LAYERS:
                if s == 0:
                    load(p, l, t).wait()
                handed(p, l, i).wait_recv()
                if p == 2:
                    passed(0, l, i).wait_recv()
                if p == 3:
                    passed(1, l, i).wait_recv()
                    passed(2, l, i).wait_recv()
                add(p, l, i)
                if p < 3:
                    passed(p, l, i).start()
                    if s + size == g[t].shape[2]:
                        load(p + 1, l, t).start()
        if p == 2:
            for copy in state():
                copy.start()

    def sent(t, blocks, sem):
        part = new[t].at[:, pl.ds(0, blocks)]
        pltpu.make_async_copy(part, part, sem).wait()

    for t in range(3):
        sent(t, 4, d2d_send.at[0, t])
        sent(t, 3, ici_send.at[0, t])

    def told(k):
        return remote(squares.at[me], squares.at[me], sq_send.at[k], sq_recv.at[k], (me + k) % n)

    squares[me] = jnp.sum(total[...], axis=0, keepdims=True)
    for k in sorted(range(1, n), key=lambda k: -min(k, n - k)):
        told(k).start()
    for copy in state():
        copy.wait()
    for k in range(1, n):
        told(k).wait_recv()
    everything = squares[0]
    for k in range(1, n):
        everything = everything + squares[k]
    everything = jnp.sum(everything, axis=(0, 1), keepdims=True)
    factor = jnp.minimum(1.0, 0.5 * lax.rsqrt(everything / count + 1e-30))

    def kind(q, last, i):
        return 0 if q < last else 2 if i in left else 1

    def spread(q, l, i):
        t, s, size = chunks[i]
        block = (chip, chip, sides[l])[q]
        part = (l, at(block), pl.ds(s, size))
        to = (sides[1 - l], sides[l], sides[1 - l])[q]
        return remote(new[t].at[part], new[t].at[part], ici_send.at[kind(q, 2, i), t], ici_recv.at[q, l, i], at(to))

    def came(q, l):
        return (sides[l], sides[1 - l], far)[q]

    def share(q, l, i):
        t, s, size = chunks[i]
        block = chip if q == 0 else came(q - 1, l)
        part = (l, at(block), pl.ds(s, size))
        arrived = d2d_recv.at[3, l, i] if q == 3 else d2d_recv.at[0, 0, t]
        return remote(new[t].at[part], new[t].at[part], d2d_send.at[kind(q, 3, i), t], arrived, partner)

    def keep(l, i):
        t, s, size = chunks[i]
        first = sum(chunks[k][2] for k in left if k < i)

        @pl.loop(0, size)
        def _(r):
            piece[first + r] = new[t][l, at(sides[l]), s + r]

    def passes(l, i, action):
        if i in left:
            pl.when(core == l)(action)
        else:
            action()

    for i, (t, s, size) in enumerate(chunks):
        for l in LAYERS:

            @pl.loop(s, s + size)
            def _(r, t=t, l=l):
                grad = new[t][l, me, r].astype(F32) * factor
                m1 = 0.9 * m[t][l, r] + 0.1 * grad
                v1 = 0.95 * v[t][l, r] + 0.05 * grad * grad
                w0 = old[t][l, r].astype(F32)
                step = m1 * lax.rsqrt(v1 + 1e-8) + 0.1 * w0
                new[t][l, me, r] = (w0 - 0.02 * step).astype(BF16)
                m[t][l, r] = m1
                v[t][l, r] = v1

            spread(0, l, i).start()
            share(0, l, i).start()
    for i in range(len(chunks)):
        for l in LAYERS:
            spread(1, l, i).start()
    for k in range(1, n):
        told(k).wait_send()
    for q in range(3):
        for i in range(len(chunks)):
            for l in LAYERS:

                def arrival(q=q, l=l, i=i):
                    spread(q, l, i).wait_recv()
                    share(q + 1, l, i).start()

                if q < 2:
                    spread(q, l, i).wait_recv()
                    if q == 0:
                        passes(l, i, lambda l=l, i=i: spread(2, l, i).start())
                    share(q + 1, l, i).start()
                    if q == 0 and i in left:
                        pl.when(core != l)(lambda l=l, i=i: keep(l, i))
                else:
                    passes(l, i, arrival)
        if q == 1:
            for t in range(3):
                sent(t, 2, ici_send.at[0, t])
    for t in range(3):
        sent(t, 3, d2d_recv.at[0, 0, t])
        sent(t, 3, d2d_send.at[0, t])
    for i in range(len(chunks)):
        for l in LAYERS:
            if i in left:
                pl.when(core != l)(lambda l=l, i=i: share(3, l, i).wait_recv())
            else:
                share(3, l, i).wait_recv()
    for t in range(3):
        units = sum(chunks[i][2] for i in left if chunks[i][0] == t)
        for part, sems in ((new[t].at[:, 0, pl.ds(0, new[t].shape[2] - units)], 1), (new[t].at[0, 0, pl.ds(0, units)], 2)):
            if part.shape[-3]:
                pltpu.make_async_copy(part, part, d2d_send.at[sems, t]).wait()
                pltpu.make_async_copy(part, part, ici_send.at[sems, t]).wait()


def put_out(k, *refs):
    copies = [pltpu.make_async_copy(refs[i], refs[k + i], refs[2 * k].at[i]) for i in range(k)]
    for copy in copies:
        copy.start()
    for copy in copies:
        copy.wait()


def written(name, *arrays):
    k = len(arrays)
    size = sum(a.size * a.dtype.itemsize for a in arrays)
    return pl.pallas_call(
        functools.partial(put_out, k),
        name=name,
        out_shape=[pltpu.HBM(a.shape, a.dtype) for a in arrays],
        in_specs=[IN_VMEM] * k,
        out_specs=[IN_HBM] * k,
        scratch_shapes=[pltpu.SemaphoreType.DMA((k,))],
        cost_estimate=pl.CostEstimate(flops=100 * size, bytes_accessed=size, transcendentals=0),
        compiler_params=pltpu.CompilerParams(has_side_effects=True, vmem_limit_bytes=VMEM_LIMIT),
    )(*arrays)


def patch(n, own, places, *refs):
    piece, outs, sem = refs[2], refs[3:5], refs[5]
    me = lax.axis_index("dp")
    far, core = (me // 2 + 2) % (n // 2), me % 2
    of = core if own else 1 - core
    copies, first = [], 0
    for k, (t, s, size) in enumerate(places):
        copies.append(pltpu.make_async_copy(piece.at[pl.ds(first, size)], outs[t].at[1 - of, far * 2 + of, pl.ds(s, size)], sem.at[k]))
        first += size
    for copy in copies:
        copy.start()
    for copy in copies:
        copy.wait()


def patched(name, n, own, places, outs, piece):
    return pl.pallas_call(
        functools.partial(patch, n, own, places),
        name=name,
        out_shape=[pltpu.HBM(o.shape, BF16) for o in outs],
        in_specs=[IN_HBM] * 2 + [IN_VMEM],
        out_specs=[IN_HBM] * 2,
        scratch_shapes=[pltpu.SemaphoreType.DMA((len(places),))],
        input_output_aliases={0: 0, 1: 1},
        cost_estimate=pl.CostEstimate(flops=100 * piece.size, bytes_accessed=2 * piece.size, transcendentals=0),
        compiler_params=pltpu.CompilerParams(has_side_effects=True, vmem_limit_bytes=VMEM_LIMIT),
    )(*outs, pltpu.with_memory_space_constraint(piece, pltpu.VMEM))


IN_VMEM, IN_HBM = pl.BlockSpec(memory_space=pltpu.VMEM), pl.BlockSpec(memory_space=pltpu.HBM)


def solution(mesh):
    n = mesh.shape["dp"]
    chips = n // 2
    ring = [(2 * c + k, 2 * ((c + (chips - 1, 1)[k]) % chips) + k) for c in range(chips) for k in range(2)]
    swap = [(d, d + 1 - 2 * (d % 2)) for d in range(n)]

    def step(*arrays):
        terms, weights, ms, vs = (arrays[i : i + 3] for i in (0, 3, 6, 9))
        layers = weights[0].shape[0]
        units = [one.shape[1] // ROWS for one in ms]
        cols = [one.shape[2] for one in ms]
        sums, chunks, left = chunks_of(units)
        count = n * sum(one.size for one in ms)
        whole = [(layers, n, u, ROWS, c) for u, c in zip(units, cols)]
        part = [(layers, u, ROWS, c) for u, c in zip(units, cols)]
        over = (sum(chunks[i][2] for i in left), ROWS, cols[0])
        operands = (
            [t.reshape(s) for t, s in zip(terms, whole)]
            + [x.reshape(s) for x, s in zip(weights, whole)]
            + [x.reshape(s) for x, s in zip(ms, part)]
            + [x.reshape(s) for x, s in zip(vs, part)]
        )
        k = max(len(sums), len(chunks))
        dma = pltpu.SemaphoreType.DMA
        outs = pl.pallas_call(
            functools.partial(kernel, n, count, sums, chunks, left),
            name="step",
            out_shape=[pltpu.VMEM(s, BF16) for s in whole] + [pltpu.VMEM(s, F32) for s in part] * 2 + [pltpu.VMEM(over, BF16)],
            in_specs=[IN_HBM] * 12,
            out_specs=[IN_VMEM] * 10,
            scratch_shapes=[pltpu.VMEM((2, *s[1:]), BF16) for s in part]
            + [pltpu.VMEM(s, BF16) for s in part]
            + [pltpu.VMEM((ROWS, 128), F32), pltpu.VMEM((n, 1, 128), F32)]
            + [dma((3, 3)), dma((4, 2, k)), dma((3, 3)), dma((3, 2, k)), dma((2, 3)), dma((3, 3)), dma((n,)), dma((n,))],
            compiler_params=pltpu.CompilerParams(collective_id=0, has_side_effects=True, vmem_limit_bytes=VMEM_LIMIT),
        )(*[pltpu.with_memory_space_constraint(o, pltpu.HBM) for o in operands])
        over = lax.ppermute(outs[9], "dp", ring)
        early, late = outs[: 9 - 1], outs[9 - 1 : 9]
        outs = list(written("put_out", *early))
        over = lax.optimization_barrier((over, outs[-1]))[0]
        across = lax.ppermute(over, "dp", swap)
        places = [chunks[i] for i in left]
        outs[:2] = patched("patch_own", n, True, places, outs[:2], over)
        outs += written("put_late", *late)
        outs[:2] = patched("patch_partner", n, False, places, outs[:2], across)
        shapes = [x.shape for x in weights] + [x.shape for x in ms] * 2
        return tuple(o.reshape(s) for o, s in zip(outs, shapes))

    all_of, cut = P(None, None, None), P(None, "dp", None)
    return jax.shard_map(
        step,
        mesh=mesh,
        in_specs=(P(("rep", "dp"), None, None, None),) * 3 + (all_of,) * 3 + (cut,) * 6,
        out_specs=(P("rep", None, None),) * 3 + (P("rep", "dp", None),) * 6,
        check_vma=False,
    )
```
